32 devices in a mesh: grp: 2 (over x), rep: 8 (over z, y), blk: 2 (over core).
Axes of the slice: x: 2, y: 2, z: 4, core: 2. Of those that a mesh axis runs over, the one named last changes fastest.
Arguments:
- factors: float32 [16, 1280, 1280], P('grp', ('blk', 'rep')), as said below
- damping: float32 [16], P('grp'), may hold values from 0.1 to 1
Outputs:
- root: float32 [16, 1280, 1280], P('grp', ('blk', 'rep'))
- inv_root: float32 [16, 1280, 1280], P('grp', ('blk', 'rep'))
The draws below stay inside these ranges and needn't reach their ends.
Inputs may be any that keep to these rules, and one draw needn't show every extreme that they name: `factors`: every factor is symmetric positive semidefinite.
All inputs are finite; a program needn't handle non-finite values.
Results may differ from the reference program's by a relative error of at most 0.0035.
The reference program's roundings to bfloat16 on the way (of `step_mat`) count: a program that leaves them out, or rounds other values in their place, can miss the bound.
Values may be sent and summed in bfloat16 or wider, within the bound.
A program may use at most 128 MiB of HBM per device.

```python
import math
import jax
import jax.numpy as jnp
from jax import lax

N = 1280
ITERS = 4
FACTORS = 16


def draw_factors(key, part):
    mix_key, scale_key = jax.random.split(jax.random.fold_in(key, 11))
    mixing = jax.random.normal(mix_key, (FACTORS, N, N), jnp.float32)
    spectrum = jnp.exp(jax.random.uniform(scale_key, (FACTORS, N), jnp.float32, jnp.log(0.001), jnp.log(10.0)))
    weighted = mixing * spectrum[:, None, :]
    product = jnp.einsum('fik,fjk->fij', weighted, mixing, precision=lax.Precision.HIGHEST) / N
    return 0.5 * (product + jnp.swapaxes(product, 1, 2))


def levels(rng, dims, pieces, least, top_value):
    def one(position, blocks):
        steps = jax.random.uniform(jax.random.fold_in(jax.random.fold_in(rng, 6), position), (blocks,), jnp.float32, least / len(pieces), top_value / len(pieces))
        return jnp.repeat(jnp.exp(steps), dims[position] // blocks).reshape((-1,) + (1,) * (len(dims) - position - 1))

    loudness = one(*pieces[0])
    for cut in pieces[1:]:
        loudness = loudness * one(*cut)
    return loudness


def setup_inputs(seed: int = 0) -> dict:
    key_of = jax.random.split(jax.random.key(seed), 3)
    factors = draw_factors(jax.random.fold_in(key_of[2], 71), 0)
    damping = jnp.clip(jnp.exp(math.log(1.0) - 2.3025851 * jax.random.uniform(key_of[1], (FACTORS,), jnp.float32) ** levels(key_of[1], (FACTORS,), ((0, 2),), -0.2, 0.2)), 0.1, 1.0)
    return dict(factors=factors, damping=damping)


def one_factor(factor_pair):
    factor, damp_value = factor_pair
    identity = jnp.eye(N, dtype=jnp.float32)
    damped = factor + damp_value * identity
    frob_norm = jnp.sqrt(jnp.sum(damped * damped))
    iterate = (damped / frob_norm).astype(jnp.bfloat16)
    inverse = identity.astype(jnp.bfloat16)
    for sweep_idx in range(ITERS):
        moment = jnp.dot(inverse, iterate, preferred_element_type=jnp.float32)
        step_mat = ((3.0 * identity - moment) * 0.5).astype(jnp.bfloat16)
        new_iterate = jnp.dot(iterate, step_mat, preferred_element_type=jnp.float32).astype(jnp.bfloat16)
        inverse = jnp.dot(step_mat, inverse, preferred_element_type=jnp.float32).astype(jnp.bfloat16)
        iterate = new_iterate
    root_scale = jnp.sqrt(frob_norm)
    return (iterate.astype(jnp.float32) * root_scale, inverse.astype(jnp.float32) / root_scale)

def reference(factors, damping):
    root, inv_root = lax.map(one_factor, (factors, damping))
    return (root, inv_root)
```

```python
import functools

import jax
import jax.numpy as jnp
from jax import lax
from jax.experimental import pallas as pl
from jax.experimental.pallas import tpu as pltpu
from jax.sharding import PartitionSpec as P

ITERS = 4
LANES = 128
CHUNK = 256
MESH = pl.DeviceIdType.MESH


def kernel(
    reps, fac_hbm, damp_ref,
    root_ref, inv_ref, norm_ref,
    fac, part, scale, send_buf, full, z1, step, near_y, last_root, last_inv,
    load_sem, sum_send, sum_recv, in_send, in_recv, fwd_send, fwd_recv,
    ex_send, ex_recv, root_send, root_recv, inv_send, inv_recv,
):
    grp = lax.axis_index("grp")
    rep = lax.axis_index("rep")
    blk = lax.axis_index("blk")
    facs, rows, order = fac.shape
    half = rows * reps
    members = 2 * reps
    rank = blk * reps + rep
    chunks = order // CHUNK
    f32, bf16 = jnp.float32, jnp.bfloat16

    side_reps = reps // 2
    side = rep // side_reps
    place = lax.rem(rep, side_reps)
    slots = facs // side_reps
    held = full.shape[0] // slots

    def factor_of(j, r):
        return j * side_reps + lax.rem(r, side_reps)

    def remote(src, dst, send, recv, r, b):
        return pltpu.make_async_remote_copy(
            src_ref=src, dst_ref=dst, send_sem=send, recv_sem=recv,
            device_id=(grp, r, b), device_id_type=MESH,
        )

    def member(j):
        q = lax.rem(rank + j, members)
        return lax.rem(q, reps), q // reps

    loads = [
        pltpu.make_async_copy(fac_hbm.at[f], fac.at[f], load_sem.at[f]) for f in range(facs)
    ]
    for load in loads:
        load.start()
    barrier = pltpu.get_barrier_semaphore()
    for j in range(1, members):
        r, b = member(j)
        pl.semaphore_signal(barrier, inc=1, device_id=(grp, r, b), device_id_type=MESH)

    row_ids = rank * rows + lax.broadcasted_iota(jnp.int32, (rows, order), 0)
    diag = row_ids == lax.broadcasted_iota(jnp.int32, (rows, order), 1)

    def damped(f):
        return fac[f] + jnp.where(diag, damp_ref[f], 0.0)

    for f in range(facs):
        loads[f].wait()
        x = damped(f)
        col = jnp.sum(x * x, axis=0, keepdims=True)
        acc = col[:, :LANES]
        for c in range(1, order // LANES):
            acc = acc + col[:, c * LANES : (c + 1) * LANES]
        part[pl.ds(rank, 1), f : f + 1, :] = acc[None]
    pl.semaphore_wait(barrier, members - 1)

    sums = []
    for j in range(1, members):
        r, b = member(j)
        copy = remote(part.at[rank], part.at[rank], sum_send.at[j], sum_recv.at[j], r, b)
        copy.start()
        sums.append(copy)
    for copy in sums:
        copy.wait()
    total = part[0]
    for q in range(1, members):
        total = total + part[q]
    norm = jnp.sqrt(jnp.sum(total, axis=1, keepdims=True))
    norm_ref[...] = jnp.broadcast_to(norm, norm_ref.shape)
    scale[...] = jnp.broadcast_to(1.0 / norm, scale.shape)

    def block_rows(b, r):
        return pl.ds(pl.multiple_of((b * reps + r) * rows, rows), rows)

    wide = -(-(half // 2) // LANES) * LANES
    narrow = half - wide

    def target(k):
        if k <= side_reps:
            return (1 - side) * side_reps + lax.rem(rep + k, side_reps)
        return side * side_reps + lax.rem(rep + k, side_reps)

    def source(k):
        if k == 0:
            return rep
        back = lax.rem(rep - k + reps, side_reps)
        if k <= side_reps:
            return (1 - side) * side_reps + back
        return side * side_reps + back

    tiles = half // LANES
    widths = sorted({tiles - (r * rows) // LANES for r in range(side_reps, reps)})

    def width_of(r, owner_side):
        mirrored = r + owner_side * (reps - 1 - 2 * r)
        return tiles - (mirrored * rows) // LANES

    def pieces(k, src, owner_side):
        if k == 0 or k > side_reps:
            return [(None, [pl.ds(0, order)])]
        options = []
        for w in widths:
            first = (1 - owner_side) * (half - w * LANES)
            options.append((
                width_of(src, owner_side) == w,
                [pl.ds(pl.multiple_of(h * half + first, LANES), w * LANES) for h in range(2)],
            ))
        return options

    def each(options, act):
        for condition, columns in options:
            if condition is None:
                act(columns)
            else:
                pl.when(condition)(functools.partial(act, columns))

    own_rows = block_rows(blk, rep)
    far_ks = list(range(1, side_reps + 1))
    near_ks = list(range(side_reps + 1, reps))

    def start_of(j):
        return full.at[j * held]

    def in_copy(j, k, i, c):
        p = target(k)
        return remote(
            send_buf.at[factor_of(j, p), :, c], start_of(j).at[own_rows, c],
            in_send.at[j, k, i], in_recv.at[j, k, i], p, blk,
        )

    def send_in(j, k, columns):
        for i, c in enumerate(columns):
            in_copy(j, k, i, c).start()

    def wait_in(j, k, columns):
        for i, c in enumerate(columns):
            in_copy(j, k, i, c).wait_send()

    for j in range(slots):
        for k in far_ks:
            p = factor_of(j, target(k))
            rounded = (damped(p) * scale[pl.ds(p, 1), 0:1]).astype(bf16)
            send_buf[p] = rounded
            if k == side_reps:
                start_of(j)[own_rows, :] = rounded
            each(pieces(k, rep, 1 - side), functools.partial(send_in, j, k))
        for k in near_ks:
            each(pieces(k, rep, 1 - side), functools.partial(send_in, j, k))

    def forward_copy(j, k, i, c):
        at = block_rows(blk, source(k))
        y0 = start_of(j)
        return remote(
            y0.at[at, c], y0.at[at, c], fwd_send.at[j, k, i], fwd_recv.at[j, k, i],
            rep, 1 - blk,
        )

    def forward(j, k, columns):
        for i, c in enumerate(columns):
            if k:
                in_copy(j, k, i, c).wait_recv()
            forward_copy(j, k, i, c).start()

    def wait_forward(j, k, columns):
        for i, c in enumerate(columns):
            forward_copy(j, k, i, c).wait()

    def forward_all(j):
        for k in [0] + near_ks + far_ks:
            each(pieces(k, source(k), side), functools.partial(forward, j, k))

    far = half // 2
    miss = half - min(widths) * LANES

    def fill(t, old, row0, col0, mirrored):
        shape = (far, miss)
        r = (row0 + lax.broadcasted_iota(jnp.int32, shape, 0)) // rows
        c = (col0 + lax.broadcasted_iota(jnp.int32, shape, 1)) // LANES
        if mirrored:
            gone = c >= tiles - ((reps - 1 - r) * rows) // LANES
        else:
            gone = c < (r * rows) // LANES
        return jnp.where(gone, t, old.astype(f32)).astype(bf16)

    mine = pl.ds(pl.multiple_of(blk * half, half), half)
    my_cols = pl.ds(pl.multiple_of(blk * half, LANES), half)
    near_rows = pl.ds(pl.multiple_of(side * far, far), far)
    eye_rows = blk * half + lax.broadcasted_iota(jnp.int32, (half, CHUNK), 0)
    eye_cols = lax.broadcasted_iota(jnp.int32, (half, CHUNK), 1)

    def cols(n):
        return slice(n * CHUNK, (n + 1) * CHUNK)

    def inv_copy(j, k):
        p = target(k)
        at = pl.ds(pl.multiple_of(lax.rem(p, side_reps) * rows, rows), rows)
        return remote(
            last_inv.at[j, at], inv_ref.at[factor_of(j, rep)],
            inv_send.at[j, k], inv_recv.at[j, k], p, blk,
        )

    def root_rows(b, r):
        first = b * wide + side * (far - narrow) + lax.rem(r, side_reps) * rows
        return pl.ds(pl.multiple_of(first, 16), rows)

    def root_copy(j, k, flip):
        r = target(k) if k else rep
        b = blk + flip - 2 * blk * flip
        return remote(
            last_root.at[j, root_rows(b, r)], root_ref.at[factor_of(j, rep), :, my_cols],
            root_send.at[j, k, flip], root_recv.at[j, k, flip], r, b,
        )

    root_ks = [(k, flip) for k in near_ks for flip in range(2)] + [(0, 1)]

    def iterate(j, carry):
        for k in range(reps):
            each(pieces(k, source(k), side), functools.partial(wait_forward, j, k))
        y0 = start_of(j)

        @pl.when(side == 0)
        def _():
            for hi in range(2):
                for hj in range(2):
                    t = y0[hj * half : hj * half + miss, hi * half + narrow : (hi + 1) * half]
                    at = (
                        slice(hi * half + far, (hi + 1) * half),
                        slice(hj * half, hj * half + miss),
                    )
                    t = t.astype(f32).T[far - narrow :, :]
                    y0[at] = fill(t, y0[at], far, 0, False)

        @pl.when(side == 1)
        def _():
            for hi in range(2):
                for hj in range(2):
                    t = y0[(hj + 1) * half - miss : (hj + 1) * half, hi * half : hi * half + wide]
                    at = (
                        slice(hi * half, hi * half + far),
                        slice((hj + 1) * half - miss, (hj + 1) * half),
                    )
                    t = t.astype(f32).T[:far, :]
                    y0[at] = fill(t, y0[at], 0, half - miss, True)

        for q in range(members):
            at = slice(q * rows, (q + 1) * rows)
            ids = q * rows + lax.broadcasted_iota(jnp.int32, (rows, order), 0)
            eye = ids == lax.broadcasted_iota(jnp.int32, (rows, order), 1)
            z1[at, :] = ((jnp.where(eye, 3.0, 0.0) - y0[at, :].astype(f32)) * 0.5).astype(bf16)

        pending = []

        def share(dst, ex, n):
            view = dst.at[mine, pl.ds(n * CHUNK, CHUNK)]
            copy = remote(view, view, ex_send.at[j, ex, n], ex_recv.at[j, ex, n], rep, 1 - blk)
            copy.start()
            pending.append(copy)
            return copy

        def product(lhs, rhs, arrivals, n):
            if arrivals is not None:
                arrivals[n].wait_recv()
            return jnp.dot(lhs, rhs[:, cols(n)], preferred_element_type=f32)

        def advance(lhs, rhs, arrivals, dst, ex):
            shared = []
            for n in range(chunks):
                dst[mine, cols(n)] = product(lhs[...], rhs, arrivals, n).astype(bf16)
                shared.append(share(dst, ex, n))
            return shared

        def make_step(y, z, arrivals):
            for n in range(chunks):
                moment = product(y[mine, :], z, arrivals, n)
                eye = jnp.where(eye_rows == eye_cols + n * CHUNK, 3.0, 0.0)
                step[:, cols(n)] = ((eye - moment) * 0.5).astype(bf16)

        base = j * held
        y, z, z_in = full.at[base + 1], z1, None
        y_in = advance(z1.at[mine], y0, None, y, 0)
        slot, ex = 2, 1
        for _ in range(ITERS - 2):
            make_step(y, z, z_in)
            z_next, y_next = full.at[base + slot], full.at[base + slot + 1]
            z_in_next = advance(step, z, None, z_next, ex)
            y_in = advance(step, y, y_in, y_next, ex + 1)
            y, z, z_in = y_next, z_next, z_in_next
            slot, ex = slot + 2, ex + 2
        make_step(y, z, z_in)

        for n in range(chunks):
            last_inv[j, :, cols(n)] = product(step[near_rows, :], z, None, n).astype(bf16)
        for k in near_ks:
            inv_copy(j, k).start()

        @pl.when(j + 1 < slots)
        def _():
            forward_all(j + 1)

        for copy in y_in:
            copy.wait_recv()
        for h in range(2):
            at = pl.ds(pl.multiple_of(h * half + side * narrow, LANES), wide)
            near_y[:, h * wide : (h + 1) * wide] = y[:, at]
        for n in range(2 * wide // CHUNK):
            out = product(step[...], near_y, None, n)
            last_root[j, cols(n), :] = out.T.astype(bf16)
        for k, flip in root_ks:
            root_copy(j, k, flip).start()
        own = factor_of(j, rep)
        local = pl.ds(pl.multiple_of(place * rows, rows), rows)
        inv_ref[own] = last_inv[j, local, :]
        root_ref[own, :, my_cols] = last_root[j, root_rows(blk, rep), :]
        for copy in pending:
            copy.wait_send()
        return carry

    forward_all(0)
    lax.fori_loop(0, slots, iterate, 0)

    for j in range(slots):
        for k in range(1, reps):
            each(pieces(k, rep, 1 - side), functools.partial(wait_in, j, k))
    for j in range(slots):
        for k in near_ks:
            inv_copy(j, k).wait()
        for k, flip in root_ks:
            root_copy(j, k, flip).wait()


def fused(mesh, factors, damping):
    facs, rows, order = factors.shape
    reps = mesh.shape["rep"]
    members = 2 * reps
    half = rows * reps
    chunks = order // CHUNK
    slots = 2
    wide = -(-(half // 2) // LANES) * LANES
    dma = pltpu.SemaphoreType.DMA
    vmem = pl.BlockSpec(memory_space=pltpu.VMEM)
    exchanges = 2 * ITERS - 3
    bf16 = jnp.bfloat16
    root, inv, norm = pl.pallas_call(
        functools.partial(kernel, reps),
        out_shape=(
            jax.ShapeDtypeStruct(factors.shape, bf16),
            jax.ShapeDtypeStruct(factors.shape, bf16),
            jax.ShapeDtypeStruct((facs, LANES), jnp.float32),
        ),
        in_specs=[
            pl.BlockSpec(memory_space=pl.ANY),
            pl.BlockSpec(memory_space=pltpu.SMEM),
        ],
        out_specs=(vmem, vmem, vmem),
        scratch_shapes=[
            pltpu.VMEM(factors.shape, jnp.float32),
            pltpu.VMEM((members, facs, LANES), jnp.float32),
            pltpu.VMEM((facs, LANES), jnp.float32),
            pltpu.VMEM(factors.shape, bf16),
            pltpu.VMEM((slots * (2 * ITERS - 2), order, order), bf16),
            pltpu.VMEM((order, order), bf16),
            pltpu.VMEM((half, order), bf16),
            pltpu.VMEM((order, 2 * wide), bf16),
            pltpu.VMEM((slots, 2 * wide, half), bf16),
            pltpu.VMEM((slots, half // 2, order), bf16),
            dma((facs,)),
            dma((members,)), dma((members,)),
            dma((slots, reps, 2)), dma((slots, reps, 2)),
            dma((slots, reps, 2)), dma((slots, reps, 2)),
            dma((slots, exchanges, chunks)), dma((slots, exchanges, chunks)),
            dma((slots, reps, 2)), dma((slots, reps, 2)),
            dma((slots, reps)), dma((slots, reps)),
        ],
        compiler_params=pltpu.CompilerParams(
            collective_id=0, has_side_effects=True, vmem_limit_bytes=63 * 2**20
        ),
    )(factors, damping)
    root_scale = jnp.sqrt(norm[:, :1])[:, :, None]
    return root.astype(jnp.float32) * root_scale, inv.astype(jnp.float32) / root_scale


def plain(factors, damping):
    fac_grp, row_count, order_full = factors.shape
    rep_count = lax.axis_size("rep")
    fac_rep = fac_grp // rep_count
    blk_rows = row_count * rep_count
    blk_idx = lax.axis_index("blk")
    rep_idx = lax.axis_index("rep")
    row_ids = blk_idx * blk_rows + rep_idx * row_count + lax.iota(jnp.int32, row_count)
    col_ids = lax.iota(jnp.int32, order_full)
    eye_block = (row_ids[:, None] == col_ids[None, :]).astype(jnp.float32)
    damped = factors + damping[:, None, None] * eye_block[None, :, :]
    factor_norms = jnp.sqrt(lax.psum(jnp.sum(damped * damped, axis=(1, 2)), ("rep", "blk")))
    own_rows = lax.all_to_all(damped, "rep", split_axis=0, concat_axis=1, tiled=True)
    own_norms = lax.dynamic_slice_in_dim(factor_norms, rep_idx * fac_rep, fac_rep)
    iterate = (own_rows / own_norms[:, None, None]).astype(jnp.bfloat16)
    iter_rows = blk_idx * blk_rows + lax.iota(jnp.int32, blk_rows)
    eye_rows = (iter_rows[:, None] == col_ids[None, :]).astype(jnp.float32)
    inverse = eye_rows[None, :, :].astype(jnp.bfloat16)
    for _ in range(ITERS):
        whole_iter = lax.all_gather(iterate, "blk", axis=1, tiled=True)
        whole_inv = lax.all_gather(inverse, "blk", axis=1, tiled=True)
        eye_full = jnp.eye(order_full, dtype=jnp.float32)
        moment = jnp.einsum(
            "fik,fkj->fij", whole_inv, whole_iter, preferred_element_type=jnp.float32
        )
        step = ((3.0 * eye_full[None, :, :] - moment) * 0.5).astype(jnp.bfloat16)
        step_rows = lax.dynamic_slice_in_dim(step, blk_idx * blk_rows, blk_rows, 1)
        new_iterate = jnp.einsum("fik,fkj->fij", iterate, step, preferred_element_type=jnp.float32)
        new_inverse = jnp.einsum(
            "fik,fkj->fij", step_rows, whole_inv, preferred_element_type=jnp.float32
        )
        iterate = new_iterate.astype(jnp.bfloat16)
        inverse = new_inverse.astype(jnp.bfloat16)
    root = lax.all_to_all(iterate, "rep", split_axis=1, concat_axis=0, tiled=True)
    inv = lax.all_to_all(inverse, "rep", split_axis=1, concat_axis=0, tiled=True)
    root_scale = jnp.sqrt(factor_norms)[:, None, None]
    return root.astype(jnp.float32) * root_scale, inv.astype(jnp.float32) / root_scale


def solution(mesh):
    def per_device(factors, damping):
        facs, rows, order = factors.shape
        if (
            facs == mesh.shape["rep"]
            and mesh.shape["blk"] == 2
            and rows % 16 == 0
            and facs % 2 == 0
            and (rows * facs) % LANES == 0
            and 2 * -(-(rows * facs // 2) // LANES) * LANES % CHUNK == 0
            and order % CHUNK == 0
        ):
            return fused(mesh, factors, damping)
        return plain(factors, damping)

    return jax.shard_map(
        per_device,
        mesh=mesh,
        in_specs=(P("grp", ("blk", "rep"), None), P("grp")),
        out_specs=(P("grp", ("blk", "rep"), None), P("grp", ("blk", "rep"), None)),
        check_vma=False,
    )
```

```python
import functools

import jax
import jax.numpy as jnp
from jax import lax
from jax.experimental import pallas as pl
from jax.experimental.pallas import tpu as pltpu
from jax.sharding import PartitionSpec as P

ITERS = 4
LANES = 128
CHUNK = 256
MESH = pl.DeviceIdType.MESH


def kernel(
    reps, fac_hbm, damp_ref,
    root_ref, inv_ref, norm_ref,
    fac, part, scale, send_buf, start, held, z1, step, near_y, last_root, last_inv,
    load_sem, sum_send, sum_recv, in_send, in_recv, fwd_send, fwd_recv,
    ex_send, ex_recv, root_send, root_recv, inv_send, inv_recv,
):
    grp = lax.axis_index("grp")
    rep = lax.axis_index("rep")
    blk = lax.axis_index("blk")
    facs, rows, order = fac.shape
    half = rows * reps
    members = 2 * reps
    rank = blk * reps + rep
    chunks = order // CHUNK
    f32, bf16 = jnp.float32, jnp.bfloat16

    side_reps = reps // 2
    side = rep // side_reps
    place = lax.rem(rep, side_reps)
    slots = facs // side_reps

    def factor_of(j, r):
        return j * side_reps + lax.rem(r, side_reps)

    def remote(src, dst, send, recv, r, b):
        return pltpu.make_async_remote_copy(
            src_ref=src, dst_ref=dst, send_sem=send, recv_sem=recv,
            device_id=(grp, r, b), device_id_type=MESH,
        )

    def member(j):
        q = lax.rem(rank + j, members)
        return lax.rem(q, reps), q // reps

    loads = [
        pltpu.make_async_copy(fac_hbm.at[f], fac.at[f], load_sem.at[f]) for f in range(facs)
    ]
    for load in loads:
        load.start()
    barrier = pltpu.get_barrier_semaphore()
    for j in range(1, members):
        r, b = member(j)
        pl.semaphore_signal(barrier, inc=1, device_id=(grp, r, b), device_id_type=MESH)

    row_ids = rank * rows + lax.broadcasted_iota(jnp.int32, (rows, order), 0)
    diag = row_ids == lax.broadcasted_iota(jnp.int32, (rows, order), 1)

    def damped(f):
        return fac[f] + jnp.where(diag, damp_ref[f], 0.0)

    for f in range(facs):
        loads[f].wait()
        x = damped(f)
        col = jnp.sum(x * x, axis=0, keepdims=True)
        acc = col[:, :LANES]
        for c in range(1, order // LANES):
            acc = acc + col[:, c * LANES : (c + 1) * LANES]
        part[pl.ds(rank, 1), f : f + 1, :] = acc[None]
    pl.semaphore_wait(barrier, members - 1)

    sums = []
    for j in range(1, members):
        r, b = member(j)
        copy = remote(part.at[rank], part.at[rank], sum_send.at[j], sum_recv.at[j], r, b)
        copy.start()
        sums.append(copy)
    for copy in sums:
        copy.wait()
    total = part[0]
    for q in range(1, members):
        total = total + part[q]
    norm = jnp.sqrt(jnp.sum(total, axis=1, keepdims=True))
    norm_ref[...] = jnp.broadcast_to(norm, norm_ref.shape)
    scale[...] = jnp.broadcast_to(1.0 / norm, scale.shape)

    def block_rows(b, r):
        return pl.ds(pl.multiple_of((b * reps + r) * rows, rows), rows)

    wide = -(-(half // 2) // LANES) * LANES
    narrow = half - wide

    def target(k):
        if k <= side_reps:
            return (1 - side) * side_reps + lax.rem(rep + k, side_reps)
        return side * side_reps + lax.rem(rep + k, side_reps)

    def source(k):
        if k == 0:
            return rep
        back = lax.rem(rep - k + reps, side_reps)
        if k <= side_reps:
            return (1 - side) * side_reps + back
        return side * side_reps + back

    tiles = half // LANES
    widths = sorted({tiles - (r * rows) // LANES for r in range(side_reps, reps)})

    def width_of(r, owner_side):
        mirrored = r + owner_side * (reps - 1 - 2 * r)
        return tiles - (mirrored * rows) // LANES

    def pieces(k, src, owner_side):
        if k == 0 or k > side_reps:
            return [(None, [pl.ds(0, order)])]
        options = []
        for w in widths:
            first = (1 - owner_side) * (half - w * LANES)
            options.append((
                width_of(src, owner_side) == w,
                [pl.ds(pl.multiple_of(h * half + first, LANES), w * LANES) for h in range(2)],
            ))
        return options

    def each(options, act):
        for condition, columns in options:
            if condition is None:
                act(columns)
            else:
                pl.when(condition)(functools.partial(act, columns))

    own_rows = block_rows(blk, rep)
    far_ks = list(range(1, side_reps + 1))
    near_ks = list(range(side_reps + 1, reps))

    def start_of(j):
        return start.at[j]

    def in_copy(j, k, i, c):
        p = target(k)
        return remote(
            send_buf.at[factor_of(j, p), :, c], start_of(j).at[own_rows, c],
            in_send.at[j, k, i], in_recv.at[j, k, i], p, blk,
        )

    def send_in(j, k, columns):
        for i, c in enumerate(columns):
            in_copy(j, k, i, c).start()

    def wait_in(j, k, columns):
        for i, c in enumerate(columns):
            in_copy(j, k, i, c).wait_send()

    for j in range(slots):
        for k in far_ks:
            p = factor_of(j, target(k))
            rounded = (damped(p) * scale[pl.ds(p, 1), 0:1]).astype(bf16)
            send_buf[p] = rounded
            if k == side_reps:
                start_of(j)[own_rows, :] = rounded
            each(pieces(k, rep, 1 - side), functools.partial(send_in, j, k))
        for k in near_ks:
            each(pieces(k, rep, 1 - side), functools.partial(send_in, j, k))

    def forward_copy(j, k, i, c):
        at = block_rows(blk, source(k))
        y0 = start_of(j)
        return remote(
            y0.at[at, c], y0.at[at, c], fwd_send.at[j, k, i], fwd_recv.at[j, k, i],
            rep, 1 - blk,
        )

    def forward(j, k, columns):
        for i, c in enumerate(columns):
            if k:
                in_copy(j, k, i, c).wait_recv()
            forward_copy(j, k, i, c).start()

    def wait_forward(j, k, columns):
        for i, c in enumerate(columns):
            forward_copy(j, k, i, c).wait()

    def forward_all(j):
        for k in [0] + near_ks + far_ks:
            each(pieces(k, source(k), side), functools.partial(forward, j, k))

    far = half // 2
    miss = half - min(widths) * LANES

    def fill(t, old, row0, col0, mirrored):
        shape = (far, miss)
        r = (row0 + lax.broadcasted_iota(jnp.int32, shape, 0)) // rows
        c = (col0 + lax.broadcasted_iota(jnp.int32, shape, 1)) // LANES
        if mirrored:
            gone = c >= tiles - ((reps - 1 - r) * rows) // LANES
        else:
            gone = c < (r * rows) // LANES
        return jnp.where(gone, t, old.astype(f32)).astype(bf16)

    mine = pl.ds(pl.multiple_of(blk * half, half), half)
    my_cols = pl.ds(pl.multiple_of(blk * half, LANES), half)
    near_rows = pl.ds(pl.multiple_of(side * far, far), far)
    eye_rows = blk * half + lax.broadcasted_iota(jnp.int32, (half, CHUNK), 0)
    eye_cols = lax.broadcasted_iota(jnp.int32, (half, CHUNK), 1)

    parts = [(0, (chunks + 1) // 2), ((chunks + 1) // 2, chunks)]

    def cols(n):
        return slice(n * CHUNK, (n + 1) * CHUNK)

    def inv_copy(j, k):
        p = target(k)
        at = pl.ds(pl.multiple_of(lax.rem(p, side_reps) * rows, rows), rows)
        return remote(
            last_inv.at[j, at], inv_ref.at[factor_of(j, rep)],
            inv_send.at[j, k], inv_recv.at[j, k], p, blk,
        )

    def root_rows(b, r):
        first = b * wide + side * (far - narrow) + lax.rem(r, side_reps) * rows
        return pl.ds(pl.multiple_of(first, 16), rows)

    def root_copy(j, k, flip):
        r = target(k) if k else rep
        b = blk + flip - 2 * blk * flip
        return remote(
            last_root.at[j, root_rows(b, r)], root_ref.at[factor_of(j, rep), :, my_cols],
            root_send.at[j, k, flip], root_recv.at[j, k, flip], r, b,
        )

    root_ks = [(k, flip) for k in near_ks for flip in range(2)] + [(0, 1)]

    def iterate(j, carry):
        for k in range(reps):
            each(pieces(k, source(k), side), functools.partial(wait_forward, j, k))
        y0 = start_of(j)

        @pl.when(side == 0)
        def _():
            for hi in range(2):
                for hj in range(2):
                    t = y0[hj * half : hj * half + miss, hi * half + narrow : (hi + 1) * half]
                    at = (
                        slice(hi * half + far, (hi + 1) * half),
                        slice(hj * half, hj * half + miss),
                    )
                    t = t.astype(f32).T[far - narrow :, :]
                    y0[at] = fill(t, y0[at], far, 0, False)

        @pl.when(side == 1)
        def _():
            for hi in range(2):
                for hj in range(2):
                    t = y0[(hj + 1) * half - miss : (hj + 1) * half, hi * half : hi * half + wide]
                    at = (
                        slice(hi * half, hi * half + far),
                        slice((hj + 1) * half - miss, (hj + 1) * half),
                    )
                    t = t.astype(f32).T[:far, :]
                    y0[at] = fill(t, y0[at], 0, half - miss, True)

        for q in range(members):
            at = slice(q * rows, (q + 1) * rows)
            ids = q * rows + lax.broadcasted_iota(jnp.int32, (rows, order), 0)
            eye = ids == lax.broadcasted_iota(jnp.int32, (rows, order), 1)
            z1[at, :] = ((jnp.where(eye, 3.0, 0.0) - y0[at, :].astype(f32)) * 0.5).astype(bf16)

        pending = []

        def share(dst, ex, part):
            first, last = parts[part]
            view = dst.at[mine, pl.ds(first * CHUNK, (last - first) * CHUNK)]
            copy = remote(
                view, view, ex_send.at[j, ex, part], ex_recv.at[j, ex, part], rep, 1 - blk
            )
            copy.start()
            pending.append(copy)
            return copy

        def settle(arrivals):
            for copy in arrivals:
                copy.wait_recv()

        def product(lhs, rhs, n):
            return jnp.dot(lhs, rhs[:, cols(n)], preferred_element_type=f32)

        def advance(lhs, rhs, arrivals, dst, ex):
            settle(arrivals)
            shared = []
            for part, (first, last) in enumerate(parts):
                for n in range(first, last):
                    dst[mine, cols(n)] = product(lhs[...], rhs, n).astype(bf16)
                shared.append(share(dst, ex, part))
            return shared

        def make_step(y, z, arrivals):
            settle(arrivals)
            for n in range(chunks):
                moment = product(y[mine, :], z, n)
                eye = jnp.where(eye_rows == eye_cols + n * CHUNK, 3.0, 0.0)
                step[:, cols(n)] = ((eye - moment) * 0.5).astype(bf16)

        y, z, z_in = held[0].at[j], z1, []
        y_in = advance(z1.at[mine], y0, [], y, 0)
        ex = 1
        for _ in range(ITERS - 2):
            make_step(y, z, z_in)
            z_next, y_next = held[ex].at[j], held[ex + 1].at[j]
            z_in_next = advance(step, z, [], z_next, ex)
            y_in = advance(step, y, y_in, y_next, ex + 1)
            y, z, z_in = y_next, z_next, z_in_next
            ex = ex + 2
        make_step(y, z, z_in)

        for n in range(chunks):
            last_inv[j, :, cols(n)] = product(step[near_rows, :], z, n).astype(bf16)
        for k in near_ks:
            inv_copy(j, k).start()

        @pl.when(j + 1 < slots)
        def _():
            forward_all(j + 1)

        settle(y_in)
        for h in range(2):
            at = pl.ds(pl.multiple_of(h * half + side * narrow, LANES), wide)
            near_y[:, h * wide : (h + 1) * wide] = y[:, at]
        for n in range(2 * wide // CHUNK):
            out = product(step[...], near_y, n)
            last_root[j, cols(n), :] = out.T.astype(bf16)
        for k, flip in root_ks:
            root_copy(j, k, flip).start()
        own = factor_of(j, rep)
        local = pl.ds(pl.multiple_of(place * rows, rows), rows)
        inv_ref[own] = last_inv[j, local, :]
        root_ref[own, :, my_cols] = last_root[j, root_rows(blk, rep), :]
        for copy in pending:
            copy.wait_send()
        return carry

    forward_all(0)
    lax.fori_loop(0, slots, iterate, 0)

    for j in range(slots):
        for k in range(1, reps):
            each(pieces(k, rep, 1 - side), functools.partial(wait_in, j, k))
    for j in range(slots):
        for k in near_ks:
            inv_copy(j, k).wait()
        for k, flip in root_ks:
            root_copy(j, k, flip).wait()


def fused(mesh, factors, damping):
    facs, rows, order = factors.shape
    reps = mesh.shape["rep"]
    members = 2 * reps
    half = rows * reps
    slots = 2
    wide = -(-(half // 2) // LANES) * LANES
    dma = pltpu.SemaphoreType.DMA
    vmem = pl.BlockSpec(memory_space=pltpu.VMEM)
    exchanges = 2 * ITERS - 3
    bf16 = jnp.bfloat16
    root, inv, norm = pl.pallas_call(
        functools.partial(kernel, reps),
        out_shape=(
            jax.ShapeDtypeStruct(factors.shape, bf16),
            jax.ShapeDtypeStruct(factors.shape, bf16),
            jax.ShapeDtypeStruct((facs, LANES), jnp.float32),
        ),
        in_specs=[
            pl.BlockSpec(memory_space=pl.ANY),
            pl.BlockSpec(memory_space=pltpu.SMEM),
        ],
        out_specs=(vmem, vmem, vmem),
        scratch_shapes=[
            pltpu.VMEM(factors.shape, jnp.float32),
            pltpu.VMEM((members, facs, LANES), jnp.float32),
            pltpu.VMEM((facs, LANES), jnp.float32),
            pltpu.VMEM(factors.shape, bf16),
            pltpu.VMEM((slots, order, order), bf16),
            [pltpu.VMEM((slots, order, order), bf16) for _ in range(exchanges)],
            pltpu.VMEM((order, order), bf16),
            pltpu.VMEM((half, order), bf16),
            pltpu.VMEM((order, 2 * wide), bf16),
            pltpu.VMEM((slots, 2 * wide, half), bf16),
            pltpu.VMEM((slots, half // 2, order), bf16),
            dma((facs,)),
            dma((members,)), dma((members,)),
            dma((slots, reps, 2)), dma((slots, reps, 2)),
            dma((slots, reps, 2)), dma((slots, reps, 2)),
            dma((slots, exchanges, 2)), dma((slots, exchanges, 2)),
            dma((slots, reps, 2)), dma((slots, reps, 2)),
            dma((slots, reps)), dma((slots, reps)),
        ],
        compiler_params=pltpu.CompilerParams(
            collective_id=0, has_side_effects=True, vmem_limit_bytes=63 * 2**20
        ),
    )(factors, damping)
    root_scale = jnp.sqrt(norm[:, :1])[:, :, None]
    return root.astype(jnp.float32) * root_scale, inv.astype(jnp.float32) / root_scale


def plain(factors, damping):
    fac_grp, row_count, order_full = factors.shape
    rep_count = lax.axis_size("rep")
    fac_rep = fac_grp // rep_count
    blk_rows = row_count * rep_count
    blk_idx = lax.axis_index("blk")
    rep_idx = lax.axis_index("rep")
    row_ids = blk_idx * blk_rows + rep_idx * row_count + lax.iota(jnp.int32, row_count)
    col_ids = lax.iota(jnp.int32, order_full)
    eye_block = (row_ids[:, None] == col_ids[None, :]).astype(jnp.float32)
    damped = factors + damping[:, None, None] * eye_block[None, :, :]
    factor_norms = jnp.sqrt(lax.psum(jnp.sum(damped * damped, axis=(1, 2)), ("rep", "blk")))
    own_rows = lax.all_to_all(damped, "rep", split_axis=0, concat_axis=1, tiled=True)
    own_norms = lax.dynamic_slice_in_dim(factor_norms, rep_idx * fac_rep, fac_rep)
    iterate = (own_rows / own_norms[:, None, None]).astype(jnp.bfloat16)
    iter_rows = blk_idx * blk_rows + lax.iota(jnp.int32, blk_rows)
    eye_rows = (iter_rows[:, None] == col_ids[None, :]).astype(jnp.float32)
    inverse = eye_rows[None, :, :].astype(jnp.bfloat16)
    for _ in range(ITERS):
        whole_iter = lax.all_gather(iterate, "blk", axis=1, tiled=True)
        whole_inv = lax.all_gather(inverse, "blk", axis=1, tiled=True)
        eye_full = jnp.eye(order_full, dtype=jnp.float32)
        moment = jnp.einsum(
            "fik,fkj->fij", whole_inv, whole_iter, preferred_element_type=jnp.float32
        )
        step = ((3.0 * eye_full[None, :, :] - moment) * 0.5).astype(jnp.bfloat16)
        step_rows = lax.dynamic_slice_in_dim(step, blk_idx * blk_rows, blk_rows, 1)
        new_iterate = jnp.einsum("fik,fkj->fij", iterate, step, preferred_element_type=jnp.float32)
        new_inverse = jnp.einsum(
            "fik,fkj->fij", step_rows, whole_inv, preferred_element_type=jnp.float32
        )
        iterate = new_iterate.astype(jnp.bfloat16)
        inverse = new_inverse.astype(jnp.bfloat16)
    root = lax.all_to_all(iterate, "rep", split_axis=1, concat_axis=0, tiled=True)
    inv = lax.all_to_all(inverse, "rep", split_axis=1, concat_axis=0, tiled=True)
    root_scale = jnp.sqrt(factor_norms)[:, None, None]
    return root.astype(jnp.float32) * root_scale, inv.astype(jnp.float32) / root_scale


def solution(mesh):
    def per_device(factors, damping):
        facs, rows, order = factors.shape
        if (
            facs == mesh.shape["rep"]
            and mesh.shape["blk"] == 2
            and rows % 16 == 0
            and facs % 2 == 0
            and (rows * facs) % LANES == 0
            and 2 * -(-(rows * facs // 2) // LANES) * LANES % CHUNK == 0
            and order % CHUNK == 0
        ):
            return fused(mesh, factors, damping)
        return plain(factors, damping)

    return jax.shard_map(
        per_device,
        mesh=mesh,
        in_specs=(P("grp", ("blk", "rep"), None), P("grp")),
        out_specs=(P("grp", ("blk", "rep"), None), P("grp", ("blk", "rep"), None)),
        check_vma=False,
    )
```

```python
import functools

import jax
import jax.numpy as jnp
from jax import lax
from jax.experimental import pallas as pl
from jax.experimental.pallas import tpu as pltpu
from jax.sharding import PartitionSpec as P

ITERS = 4
LANES = 128
CHUNK = 256
MESH = pl.DeviceIdType.MESH


def kernel(
    reps, fac_hbm, damp_ref,
    root_ref, inv_ref, norm_ref,
    fac, part, scale, send_buf, start, held, z1, step, near_y, last_root, last_inv,
    load_sem, sum_send, sum_recv, in_send, in_recv, fwd_send, fwd_recv,
    ex_send, ex_recv, root_send, root_recv, inv_send, inv_recv,
):
    grp = lax.axis_index("grp")
    rep = lax.axis_index("rep")
    blk = lax.axis_index("blk")
    facs, rows, order = fac.shape
    half = rows * reps
    members = 2 * reps
    rank = blk * reps + rep
    chunks = order // CHUNK
    f32, bf16 = jnp.float32, jnp.bfloat16

    side_reps = reps // 2
    side = rep // side_reps
    place = lax.rem(rep, side_reps)
    slots = facs // side_reps

    def factor_of(j, r):
        return j * side_reps + lax.rem(r, side_reps)

    def remote(src, dst, send, recv, r, b):
        return pltpu.make_async_remote_copy(
            src_ref=src, dst_ref=dst, send_sem=send, recv_sem=recv,
            device_id=(grp, r, b), device_id_type=MESH,
        )

    def member(j):
        q = lax.rem(rank + j, members)
        return lax.rem(q, reps), q // reps

    loads = [
        pltpu.make_async_copy(fac_hbm.at[f], fac.at[f], load_sem.at[f]) for f in range(facs)
    ]
    for load in loads:
        load.start()
    barrier = pltpu.get_barrier_semaphore()
    for j in range(1, members):
        r, b = member(j)
        pl.semaphore_signal(barrier, inc=1, device_id=(grp, r, b), device_id_type=MESH)

    row_ids = rank * rows + lax.broadcasted_iota(jnp.int32, (rows, order), 0)
    diag = row_ids == lax.broadcasted_iota(jnp.int32, (rows, order), 1)

    def damped(f):
        return fac[f] + jnp.where(diag, damp_ref[f], 0.0)

    for f in range(facs):
        loads[f].wait()
        x = damped(f)
        col = jnp.sum(x * x, axis=0, keepdims=True)
        acc = col[:, :LANES]
        for c in range(1, order // LANES):
            acc = acc + col[:, c * LANES : (c + 1) * LANES]
        part[pl.ds(rank, 1), f : f + 1, :] = acc[None]
    pl.semaphore_wait(barrier, members - 1)

    sums = []
    for j in range(1, members):
        r, b = member(j)
        copy = remote(part.at[rank], part.at[rank], sum_send.at[j], sum_recv.at[j], r, b)
        copy.start()
        sums.append(copy)
    for copy in sums:
        copy.wait()
    total = part[0]
    for q in range(1, members):
        total = total + part[q]
    norm = jnp.sqrt(jnp.sum(total, axis=1, keepdims=True))
    norm_ref[...] = jnp.broadcast_to(norm, norm_ref.shape)
    scale[...] = jnp.broadcast_to(1.0 / norm, scale.shape)

    def block_rows(b, r):
        return pl.ds(pl.multiple_of((b * reps + r) * rows, rows), rows)

    wide = -(-(half // 2) // LANES) * LANES
    narrow = half - wide

    def target(k):
        if k <= side_reps:
            return (1 - side) * side_reps + lax.rem(rep + k, side_reps)
        return side * side_reps + lax.rem(rep + k, side_reps)

    def source(k):
        if k == 0:
            return rep
        back = lax.rem(rep - k + reps, side_reps)
        if k <= side_reps:
            return (1 - side) * side_reps + back
        return side * side_reps + back

    tiles = half // LANES
    widths = sorted({tiles - (r * rows) // LANES for r in range(side_reps, reps)})

    def width_of(r, owner_side):
        mirrored = r + owner_side * (reps - 1 - 2 * r)
        return tiles - (mirrored * rows) // LANES

    def pieces(k, src, owner_side):
        if k == 0 or k > side_reps:
            return [(None, [pl.ds(0, order)])]
        options = []
        for w in widths:
            first = (1 - owner_side) * (half - w * LANES)
            options.append((
                width_of(src, owner_side) == w,
                [pl.ds(pl.multiple_of(h * half + first, LANES), w * LANES) for h in range(2)],
            ))
        return options

    def each(options, act):
        for condition, columns in options:
            if condition is None:
                act(columns)
            else:
                pl.when(condition)(functools.partial(act, columns))

    own_rows = block_rows(blk, rep)
    far_ks = list(range(1, side_reps + 1))
    near_ks = list(range(side_reps + 1, reps))

    def start_of(j):
        return start.at[j]

    def in_copy(j, k, i, c):
        p = target(k)
        return remote(
            send_buf.at[factor_of(j, p), :, c], start_of(j).at[own_rows, c],
            in_send.at[j, k, i], in_recv.at[j, k, i], p, blk,
        )

    def send_in(j, k, columns):
        for i, c in enumerate(columns):
            in_copy(j, k, i, c).start()

    def wait_in(j, k, columns):
        for i, c in enumerate(columns):
            in_copy(j, k, i, c).wait_send()

    def round_rows(j, k):
        p = factor_of(j, target(k))
        rounded = (damped(p) * scale[pl.ds(p, 1), 0:1]).astype(bf16)
        send_buf[p] = rounded
        if k == side_reps:
            start_of(j)[own_rows, :] = rounded

    def send_all(j, ks):
        for k in ks:
            each(pieces(k, rep, 1 - side), functools.partial(send_in, j, k))

    for k in far_ks:
        round_rows(0, k)
        send_all(0, [k])
    send_all(0, near_ks)
    for j in range(1, slots):
        for k in far_ks:
            round_rows(j, k)

    def forward_copy(j, k, i, c):
        at = block_rows(blk, source(k))
        y0 = start_of(j)
        return remote(
            y0.at[at, c], y0.at[at, c], fwd_send.at[j, k, i], fwd_recv.at[j, k, i],
            rep, 1 - blk,
        )

    def forward(j, k, columns):
        for i, c in enumerate(columns):
            if k:
                in_copy(j, k, i, c).wait_recv()
            forward_copy(j, k, i, c).start()

    def wait_forward(j, k, columns):
        for i, c in enumerate(columns):
            forward_copy(j, k, i, c).wait()

    def forward_all(j):
        for k in [0] + near_ks + far_ks:
            each(pieces(k, source(k), side), functools.partial(forward, j, k))

    far = half // 2
    miss = half - min(widths) * LANES

    def fill(t, old, row0, col0, mirrored):
        shape = (far, miss)
        r = (row0 + lax.broadcasted_iota(jnp.int32, shape, 0)) // rows
        c = (col0 + lax.broadcasted_iota(jnp.int32, shape, 1)) // LANES
        if mirrored:
            gone = c >= tiles - ((reps - 1 - r) * rows) // LANES
        else:
            gone = c < (r * rows) // LANES
        return jnp.where(gone, t, old.astype(f32)).astype(bf16)

    mine = pl.ds(pl.multiple_of(blk * half, half), half)
    my_cols = pl.ds(pl.multiple_of(blk * half, LANES), half)
    near_rows = pl.ds(pl.multiple_of(side * far, far), far)
    eye_rows = blk * half + lax.broadcasted_iota(jnp.int32, (half, CHUNK), 0)
    eye_cols = lax.broadcasted_iota(jnp.int32, (half, CHUNK), 1)

    parts = [(0, (chunks + 1) // 2), ((chunks + 1) // 2, chunks)]

    def cols(n):
        return slice(n * CHUNK, (n + 1) * CHUNK)

    def inv_copy(j, k):
        p = target(k)
        at = pl.ds(pl.multiple_of(lax.rem(p, side_reps) * rows, rows), rows)
        return remote(
            last_inv.at[j, at], inv_ref.at[factor_of(j, rep)],
            inv_send.at[j, k], inv_recv.at[j, k], p, blk,
        )

    def root_rows(b, r):
        first = b * wide + side * (far - narrow) + lax.rem(r, side_reps) * rows
        return pl.ds(pl.multiple_of(first, 16), rows)

    def root_copy(j, k, flip):
        r = target(k) if k else rep
        b = blk + flip - 2 * blk * flip
        return remote(
            last_root.at[j, root_rows(b, r)], root_ref.at[factor_of(j, rep), :, my_cols],
            root_send.at[j, k, flip], root_recv.at[j, k, flip], r, b,
        )

    root_ks = [(k, flip) for k in near_ks for flip in range(2)] + [(0, 1)]

    def iterate(j, carry):
        for k in range(reps):
            each(pieces(k, source(k), side), functools.partial(wait_forward, j, k))
        y0 = start_of(j)

        @pl.when(j + 1 < slots)
        def _():
            send_all(j + 1, far_ks + near_ks)

        @pl.when(side == 0)
        def _():
            for hi in range(2):
                for hj in range(2):
                    t = y0[hj * half : hj * half + miss, hi * half + narrow : (hi + 1) * half]
                    at = (
                        slice(hi * half + far, (hi + 1) * half),
                        slice(hj * half, hj * half + miss),
                    )
                    t = t.astype(f32).T[far - narrow :, :]
                    y0[at] = fill(t, y0[at], far, 0, False)

        @pl.when(side == 1)
        def _():
            for hi in range(2):
                for hj in range(2):
                    t = y0[(hj + 1) * half - miss : (hj + 1) * half, hi * half : hi * half + wide]
                    at = (
                        slice(hi * half, hi * half + far),
                        slice((hj + 1) * half - miss, (hj + 1) * half),
                    )
                    t = t.astype(f32).T[:far, :]
                    y0[at] = fill(t, y0[at], 0, half - miss, True)

        for q in range(members):
            at = slice(q * rows, (q + 1) * rows)
            ids = q * rows + lax.broadcasted_iota(jnp.int32, (rows, order), 0)
            eye = ids == lax.broadcasted_iota(jnp.int32, (rows, order), 1)
            z1[at, :] = ((jnp.where(eye, 3.0, 0.0) - y0[at, :].astype(f32)) * 0.5).astype(bf16)

        pending = []

        def share(dst, ex, part):
            first, last = parts[part]
            view = dst.at[mine, pl.ds(first * CHUNK, (last - first) * CHUNK)]
            copy = remote(
                view, view, ex_send.at[j, ex, part], ex_recv.at[j, ex, part], rep, 1 - blk
            )
            copy.start()
            pending.append(copy)
            return copy

        def settle(arrivals):
            for copy in arrivals:
                copy.wait_recv()

        def product(lhs, rhs, n):
            return jnp.dot(lhs, rhs[:, cols(n)], preferred_element_type=f32)

        def advance(lhs, rhs, arrivals, dst, ex):
            settle(arrivals)
            shared = []
            for part, (first, last) in enumerate(parts):
                for n in range(first, last):
                    dst[mine, cols(n)] = product(lhs[...], rhs, n).astype(bf16)
                shared.append(share(dst, ex, part))
            return shared

        def make_step(y, z, arrivals):
            settle(arrivals)
            for n in range(chunks):
                moment = product(y[mine, :], z, n)
                eye = jnp.where(eye_rows == eye_cols + n * CHUNK, 3.0, 0.0)
                step[:, cols(n)] = ((eye - moment) * 0.5).astype(bf16)

        def make_step_rows(y, z, first, count):
            first = pl.multiple_of(first, 16)
            top = pl.multiple_of(blk * half + first, 16)
            ids = top + lax.broadcasted_iota(jnp.int32, (count, CHUNK), 0)
            for n in range(chunks):
                moment = product(y[pl.ds(top, count), :], z, n)
                at = n * CHUNK + lax.broadcasted_iota(jnp.int32, (count, CHUNK), 1)
                eye = jnp.where(ids == at, 3.0, 0.0)
                step[pl.ds(first, count), cols(n)] = ((eye - moment) * 0.5).astype(bf16)

        y, z, z_in = held[0].at[j], z1, []
        y_in = advance(z1.at[mine], y0, [], y, 0)
        ex = 1
        for _ in range(ITERS - 2):
            make_step(y, z, z_in)
            z_next, y_next = held[ex].at[j], held[ex + 1].at[j]
            z_in_next = advance(step, z, [], z_next, ex)
            y_in = advance(step, y, y_in, y_next, ex + 1)
            y, z, z_in = y_next, z_next, z_in_next
            ex = ex + 2
        settle(z_in)
        make_step_rows(y, z, side * far, far)
        for n in range(chunks):
            last_inv[j, :, cols(n)] = product(step[near_rows, :], z, n).astype(bf16)
        for k in near_ks:
            inv_copy(j, k).start()

        @pl.when(j + 1 < slots)
        def _():
            forward_all(j + 1)

        make_step_rows(y, z, (1 - side) * far, far)
        settle(y_in)
        for h in range(2):
            at = pl.ds(pl.multiple_of(h * half + side * narrow, LANES), wide)
            near_y[:, h * wide : (h + 1) * wide] = y[:, at]
        for n in range(2 * wide // CHUNK):
            out = product(step[...], near_y, n)
            last_root[j, cols(n), :] = out.T.astype(bf16)
        for k, flip in root_ks:
            root_copy(j, k, flip).start()
        own = factor_of(j, rep)
        local = pl.ds(pl.multiple_of(place * rows, rows), rows)
        inv_ref[own] = last_inv[j, local, :]
        root_ref[own, :, my_cols] = last_root[j, root_rows(blk, rep), :]
        for copy in pending:
            copy.wait_send()
        return carry

    forward_all(0)
    lax.fori_loop(0, slots, iterate, 0)

    for j in range(slots):
        for k in range(1, reps):
            each(pieces(k, rep, 1 - side), functools.partial(wait_in, j, k))
    for j in range(slots):
        for k in near_ks:
            inv_copy(j, k).wait()
        for k, flip in root_ks:
            root_copy(j, k, flip).wait()


def fused(mesh, factors, damping):
    facs, rows, order = factors.shape
    reps = mesh.shape["rep"]
    members = 2 * reps
    half = rows * reps
    slots = 2
    wide = -(-(half // 2) // LANES) * LANES
    dma = pltpu.SemaphoreType.DMA
    vmem = pl.BlockSpec(memory_space=pltpu.VMEM)
    exchanges = 2 * ITERS - 3
    bf16 = jnp.bfloat16
    root, inv, norm = pl.pallas_call(
        functools.partial(kernel, reps),
        out_shape=(
            jax.ShapeDtypeStruct(factors.shape, bf16),
            jax.ShapeDtypeStruct(factors.shape, bf16),
            jax.ShapeDtypeStruct((facs, LANES), jnp.float32),
        ),
        in_specs=[
            pl.BlockSpec(memory_space=pl.ANY),
            pl.BlockSpec(memory_space=pltpu.SMEM),
        ],
        out_specs=(vmem, vmem, vmem),
        scratch_shapes=[
            pltpu.VMEM(factors.shape, jnp.float32),
            pltpu.VMEM((members, facs, LANES), jnp.float32),
            pltpu.VMEM((facs, LANES), jnp.float32),
            pltpu.VMEM(factors.shape, bf16),
            pltpu.VMEM((slots, order, order), bf16),
            [pltpu.VMEM((slots, order, order), bf16) for _ in range(exchanges)],
            pltpu.VMEM((order, order), bf16),
            pltpu.VMEM((half, order), bf16),
            pltpu.VMEM((order, 2 * wide), bf16),
            pltpu.VMEM((slots, 2 * wide, half), bf16),
            pltpu.VMEM((slots, half // 2, order), bf16),
            dma((facs,)),
            dma((members,)), dma((members,)),
            dma((slots, reps, 2)), dma((slots, reps, 2)),
            dma((slots, reps, 2)), dma((slots, reps, 2)),
            dma((slots, exchanges, 2)), dma((slots, exchanges, 2)),
            dma((slots, reps, 2)), dma((slots, reps, 2)),
            dma((slots, reps)), dma((slots, reps)),
        ],
        compiler_params=pltpu.CompilerParams(
            collective_id=0, has_side_effects=True, vmem_limit_bytes=63 * 2**20
        ),
    )(factors, damping)
    root_scale = jnp.sqrt(norm[:, :1])[:, :, None]
    return root.astype(jnp.float32) * root_scale, inv.astype(jnp.float32) / root_scale


def plain(factors, damping):
    fac_grp, row_count, order_full = factors.shape
    rep_count = lax.axis_size("rep")
    fac_rep = fac_grp // rep_count
    blk_rows = row_count * rep_count
    blk_idx = lax.axis_index("blk")
    rep_idx = lax.axis_index("rep")
    row_ids = blk_idx * blk_rows + rep_idx * row_count + lax.iota(jnp.int32, row_count)
    col_ids = lax.iota(jnp.int32, order_full)
    eye_block = (row_ids[:, None] == col_ids[None, :]).astype(jnp.float32)
    damped = factors + damping[:, None, None] * eye_block[None, :, :]
    factor_norms = jnp.sqrt(lax.psum(jnp.sum(damped * damped, axis=(1, 2)), ("rep", "blk")))
    own_rows = lax.all_to_all(damped, "rep", split_axis=0, concat_axis=1, tiled=True)
    own_norms = lax.dynamic_slice_in_dim(factor_norms, rep_idx * fac_rep, fac_rep)
    iterate = (own_rows / own_norms[:, None, None]).astype(jnp.bfloat16)
    iter_rows = blk_idx * blk_rows + lax.iota(jnp.int32, blk_rows)
    eye_rows = (iter_rows[:, None] == col_ids[None, :]).astype(jnp.float32)
    inverse = eye_rows[None, :, :].astype(jnp.bfloat16)
    for _ in range(ITERS):
        whole_iter = lax.all_gather(iterate, "blk", axis=1, tiled=True)
        whole_inv = lax.all_gather(inverse, "blk", axis=1, tiled=True)
        eye_full = jnp.eye(order_full, dtype=jnp.float32)
        moment = jnp.einsum(
            "fik,fkj->fij", whole_inv, whole_iter, preferred_element_type=jnp.float32
        )
        step = ((3.0 * eye_full[None, :, :] - moment) * 0.5).astype(jnp.bfloat16)
        step_rows = lax.dynamic_slice_in_dim(step, blk_idx * blk_rows, blk_rows, 1)
        new_iterate = jnp.einsum("fik,fkj->fij", iterate, step, preferred_element_type=jnp.float32)
        new_inverse = jnp.einsum(
            "fik,fkj->fij", step_rows, whole_inv, preferred_element_type=jnp.float32
        )
        iterate = new_iterate.astype(jnp.bfloat16)
        inverse = new_inverse.astype(jnp.bfloat16)
    root = lax.all_to_all(iterate, "rep", split_axis=1, concat_axis=0, tiled=True)
    inv = lax.all_to_all(inverse, "rep", split_axis=1, concat_axis=0, tiled=True)
    root_scale = jnp.sqrt(factor_norms)[:, None, None]
    return root.astype(jnp.float32) * root_scale, inv.astype(jnp.float32) / root_scale


def solution(mesh):
    def per_device(factors, damping):
        facs, rows, order = factors.shape
        if (
            facs == mesh.shape["rep"]
            and mesh.shape["blk"] == 2
            and rows % 16 == 0
            and facs % 2 == 0
            and (rows * facs) % LANES == 0
            and 2 * -(-(rows * facs // 2) // LANES) * LANES % CHUNK == 0
            and order % CHUNK == 0
        ):
            return fused(mesh, factors, damping)
        return plain(factors, damping)

    return jax.shard_map(
        per_device,
        mesh=mesh,
        in_specs=(P("grp", ("blk", "rep"), None), P("grp")),
        out_specs=(P("grp", ("blk", "rep"), None), P("grp", ("blk", "rep"), None)),
        check_vma=False,
    )
```

```python
import functools

import jax
import jax.numpy as jnp
from jax import lax
from jax.experimental import pallas as pl
from jax.experimental.pallas import tpu as pltpu
from jax.sharding import PartitionSpec as P

ITERS = 4
LANES = 128
CHUNK = 256
MESH = pl.DeviceIdType.MESH


def kernel(
    reps, fac_hbm, damp_ref,
    root_hbm, inv_hbm, norm_ref,
    root_ref, inv_ref, fac, part, scale, send_buf, start, held, z1, step, near_y, last_root, last_inv,
    load_sem, sum_send, sum_recv, in_send, in_recv, fwd_send, fwd_recv,
    ex_send, ex_recv, root_send, root_recv, inv_send, inv_recv, store_sem,
):
    grp = lax.axis_index("grp")
    rep = lax.axis_index("rep")
    blk = lax.axis_index("blk")
    facs, rows, order = fac.shape
    half = rows * reps
    members = 2 * reps
    rank = blk * reps + rep
    chunks = order // CHUNK
    f32, bf16 = jnp.float32, jnp.bfloat16

    side_reps = reps // 2
    side = rep // side_reps
    place = lax.rem(rep, side_reps)
    slots = facs // side_reps

    def factor_of(j, r):
        return j * side_reps + lax.rem(r, side_reps)

    def remote(src, dst, send, recv, r, b):
        return pltpu.make_async_remote_copy(
            src_ref=src, dst_ref=dst, send_sem=send, recv_sem=recv,
            device_id=(grp, r, b), device_id_type=MESH,
        )

    def member(j):
        q = lax.rem(rank + j, members)
        return lax.rem(q, reps), q // reps

    loads = [
        pltpu.make_async_copy(fac_hbm.at[f], fac.at[f], load_sem.at[f]) for f in range(facs)
    ]
    for load in loads:
        load.start()
    barrier = pltpu.get_barrier_semaphore()
    for j in range(1, members):
        r, b = member(j)
        pl.semaphore_signal(barrier, inc=1, device_id=(grp, r, b), device_id_type=MESH)

    row_ids = rank * rows + lax.broadcasted_iota(jnp.int32, (rows, order), 0)
    diag = row_ids == lax.broadcasted_iota(jnp.int32, (rows, order), 1)

    def damped(f):
        return fac[f] + jnp.where(diag, damp_ref[f], 0.0)

    for f in range(facs):
        loads[f].wait()
        x = damped(f)
        col = jnp.sum(x * x, axis=0, keepdims=True)
        acc = col[:, :LANES]
        for c in range(1, order // LANES):
            acc = acc + col[:, c * LANES : (c + 1) * LANES]
        part[pl.ds(rank, 1), f : f + 1, :] = acc[None]
    pl.semaphore_wait(barrier, members - 1)

    sums = []
    for j in range(1, members):
        r, b = member(j)
        copy = remote(part.at[rank], part.at[rank], sum_send.at[j], sum_recv.at[j], r, b)
        copy.start()
        sums.append(copy)
    for copy in sums:
        copy.wait()
    total = part[0]
    for q in range(1, members):
        total = total + part[q]
    norm = jnp.sqrt(jnp.sum(total, axis=1, keepdims=True))
    norm_ref[...] = jnp.broadcast_to(norm, norm_ref.shape)
    scale[...] = jnp.broadcast_to(1.0 / norm, scale.shape)

    def block_rows(b, r):
        return pl.ds(pl.multiple_of((b * reps + r) * rows, rows), rows)

    wide = -(-(half // 2) // LANES) * LANES
    narrow = half - wide

    def target(k):
        if k <= side_reps:
            return (1 - side) * side_reps + lax.rem(rep + k, side_reps)
        return side * side_reps + lax.rem(rep + k, side_reps)

    def source(k):
        if k == 0:
            return rep
        back = lax.rem(rep - k + reps, side_reps)
        if k <= side_reps:
            return (1 - side) * side_reps + back
        return side * side_reps + back

    tiles = half // LANES
    widths = sorted({tiles - (r * rows) // LANES for r in range(side_reps, reps)})

    def width_of(r, owner_side):
        mirrored = r + owner_side * (reps - 1 - 2 * r)
        return tiles - (mirrored * rows) // LANES

    def pieces(k, src, owner_side):
        if k == 0 or k > side_reps:
            return [(None, [pl.ds(0, order)])]
        options = []
        for w in widths:
            first = (1 - owner_side) * (half - w * LANES)
            options.append((
                width_of(src, owner_side) == w,
                [pl.ds(pl.multiple_of(h * half + first, LANES), w * LANES) for h in range(2)],
            ))
        return options

    def each(options, act):
        for condition, columns in options:
            if condition is None:
                act(columns)
            else:
                pl.when(condition)(functools.partial(act, columns))

    own_rows = block_rows(blk, rep)
    far_ks = list(range(1, side_reps + 1))
    near_ks = list(range(side_reps + 1, reps))

    def start_of(j):
        return start.at[j]

    def in_copy(j, k, i, c):
        p = target(k)
        return remote(
            send_buf.at[factor_of(j, p), :, c], start_of(j).at[own_rows, c],
            in_send.at[j, k, i], in_recv.at[j, k, i], p, blk,
        )

    def send_in(j, k, columns):
        for i, c in enumerate(columns):
            in_copy(j, k, i, c).start()

    def wait_in(j, k, columns):
        for i, c in enumerate(columns):
            in_copy(j, k, i, c).wait_send()

    def round_rows(j, k):
        p = factor_of(j, target(k))
        rounded = (damped(p) * scale[pl.ds(p, 1), 0:1]).astype(bf16)
        send_buf[p] = rounded
        if k == side_reps:
            start_of(j)[own_rows, :] = rounded

    def send_all(j, ks):
        for k in ks:
            each(pieces(k, rep, 1 - side), functools.partial(send_in, j, k))

    for k in far_ks:
        round_rows(0, k)
        send_all(0, [k])
    send_all(0, near_ks)
    for j in range(1, slots):
        for k in far_ks:
            round_rows(j, k)

    def forward_copy(j, k, i, c):
        at = block_rows(blk, source(k))
        y0 = start_of(j)
        return remote(
            y0.at[at, c], y0.at[at, c], fwd_send.at[j, k, i], fwd_recv.at[j, k, i],
            rep, 1 - blk,
        )

    def forward(j, k, columns):
        for i, c in enumerate(columns):
            if k:
                in_copy(j, k, i, c).wait_recv()
            forward_copy(j, k, i, c).start()

    def wait_forward(j, k, columns):
        for i, c in enumerate(columns):
            forward_copy(j, k, i, c).wait()

    def forward_all(j):
        for k in [0] + near_ks + far_ks:
            each(pieces(k, source(k), side), functools.partial(forward, j, k))

    far = half // 2
    miss = half - min(widths) * LANES

    def fill(t, old, row0, col0, mirrored):
        shape = (far, miss)
        r = (row0 + lax.broadcasted_iota(jnp.int32, shape, 0)) // rows
        c = (col0 + lax.broadcasted_iota(jnp.int32, shape, 1)) // LANES
        if mirrored:
            gone = c >= tiles - ((reps - 1 - r) * rows) // LANES
        else:
            gone = c < (r * rows) // LANES
        return jnp.where(gone, t, old.astype(f32)).astype(bf16)

    mine = pl.ds(pl.multiple_of(blk * half, half), half)
    my_cols = pl.ds(pl.multiple_of(blk * half, LANES), half)
    near_rows = pl.ds(pl.multiple_of(side * far, far), far)
    eye_rows = blk * half + lax.broadcasted_iota(jnp.int32, (half, CHUNK), 0)
    eye_cols = lax.broadcasted_iota(jnp.int32, (half, CHUNK), 1)

    whole = [(0, chunks)]
    halves = [(0, (chunks + 1) // 2), ((chunks + 1) // 2, chunks)]

    def cols(n):
        return slice(n * CHUNK, (n + 1) * CHUNK)

    def inv_copy(j, k):
        p = target(k)
        at = pl.ds(pl.multiple_of(lax.rem(p, side_reps) * rows, rows), rows)
        return remote(
            last_inv.at[j, at], inv_ref.at[factor_of(j, rep)],
            inv_send.at[j, k], inv_recv.at[j, k], p, blk,
        )

    def root_rows(b, r):
        first = b * wide + side * (far - narrow) + lax.rem(r, side_reps) * rows
        return pl.ds(pl.multiple_of(first, 16), rows)

    def root_copy(j, k, flip):
        r = target(k) if k else rep
        b = blk + flip - 2 * blk * flip
        return remote(
            last_root.at[j, root_rows(b, r)], root_ref.at[factor_of(j, rep), :, my_cols],
            root_send.at[j, k, flip], root_recv.at[j, k, flip], r, b,
        )

    root_ks = [(k, flip) for k in near_ks for flip in range(2)] + [(0, 1)]

    def iterate(j, carry):
        for k in range(reps):
            each(pieces(k, source(k), side), functools.partial(wait_forward, j, k))
        y0 = start_of(j)

        @pl.when(j + 1 < slots)
        def _():
            send_all(j + 1, far_ks + near_ks)

        @pl.when(side == 0)
        def _():
            for hi in range(2):
                for hj in range(2):
                    t = y0[hj * half : hj * half + miss, hi * half + narrow : (hi + 1) * half]
                    at = (
                        slice(hi * half + far, (hi + 1) * half),
                        slice(hj * half, hj * half + miss),
                    )
                    t = t.astype(f32).T[far - narrow :, :]
                    y0[at] = fill(t, y0[at], far, 0, False)

        @pl.when(side == 1)
        def _():
            for hi in range(2):
                for hj in range(2):
                    t = y0[(hj + 1) * half - miss : (hj + 1) * half, hi * half : hi * half + wide]
                    at = (
                        slice(hi * half, hi * half + far),
                        slice((hj + 1) * half - miss, (hj + 1) * half),
                    )
                    t = t.astype(f32).T[:far, :]
                    y0[at] = fill(t, y0[at], 0, half - miss, True)

        for q in range(members):
            at = slice(q * rows, (q + 1) * rows)
            ids = q * rows + lax.broadcasted_iota(jnp.int32, (rows, order), 0)
            eye = ids == lax.broadcasted_iota(jnp.int32, (rows, order), 1)
            z1[at, :] = ((jnp.where(eye, 3.0, 0.0) - y0[at, :].astype(f32)) * 0.5).astype(bf16)

        pending = []

        def share(dst, ex, part, first, last):
            view = dst.at[mine, pl.ds(first * CHUNK, (last - first) * CHUNK)]
            copy = remote(
                view, view, ex_send.at[j, ex, part], ex_recv.at[j, ex, part], rep, 1 - blk
            )
            copy.start()
            pending.append(copy)
            return copy

        def settle(arrivals):
            for copy in arrivals:
                copy.wait_recv()

        def product(lhs, rhs, n):
            return jnp.dot(lhs, rhs[:, cols(n)], preferred_element_type=f32)

        def advance(lhs, rhs, arrivals, dst, ex, parts):
            settle(arrivals)
            shared = []
            for part, (first, last) in enumerate(parts):
                for n in range(first, last):
                    dst[mine, cols(n)] = product(lhs[...], rhs, n).astype(bf16)
                shared.append(share(dst, ex, part, first, last))
            return shared

        def make_step(y, z, arrivals):
            settle(arrivals)
            for n in range(chunks):
                moment = product(y[mine, :], z, n)
                eye = jnp.where(eye_rows == eye_cols + n * CHUNK, 3.0, 0.0)
                step[:, cols(n)] = ((eye - moment) * 0.5).astype(bf16)

        def make_step_rows(y, z, first, count):
            first = pl.multiple_of(first, 16)
            top = pl.multiple_of(blk * half + first, 16)
            ids = top + lax.broadcasted_iota(jnp.int32, (count, CHUNK), 0)
            for n in range(chunks):
                moment = product(y[pl.ds(top, count), :], z, n)
                at = n * CHUNK + lax.broadcasted_iota(jnp.int32, (count, CHUNK), 1)
                eye = jnp.where(ids == at, 3.0, 0.0)
                step[pl.ds(first, count), cols(n)] = ((eye - moment) * 0.5).astype(bf16)

        y, z, z_in = held[0].at[j], z1, []
        y_in = advance(z1.at[mine], y0, [], y, 0, whole)
        ex = 1
        for _ in range(ITERS - 2):
            make_step(y, z, z_in)
            z_next, y_next = held[ex].at[j], held[ex + 1].at[j]
            z_in_next = advance(step, z, [], z_next, ex, halves)
            y_in = advance(step, y, y_in, y_next, ex + 1, whole)
            y, z, z_in = y_next, z_next, z_in_next
            ex = ex + 2
        settle(z_in)
        make_step_rows(y, z, side * far, far)
        for n in range(chunks):
            last_inv[j, :, cols(n)] = product(step[near_rows, :], z, n).astype(bf16)
        for k in near_ks:
            inv_copy(j, k).start()

        @pl.when(j + 1 < slots)
        def _():
            forward_all(j + 1)

        make_step_rows(y, z, (1 - side) * far, far)
        settle(y_in)
        for h in range(2):
            at = pl.ds(pl.multiple_of(h * half + side * narrow, LANES), wide)
            near_y[:, h * wide : (h + 1) * wide] = y[:, at]
        for n in range(2 * wide // CHUNK):
            out = product(step[...], near_y, n)
            last_root[j, cols(n), :] = out.T.astype(bf16)
        for k, flip in root_ks:
            root_copy(j, k, flip).start()
        own = factor_of(j, rep)
        local = pl.ds(pl.multiple_of(place * rows, rows), rows)
        inv_ref[own] = last_inv[j, local, :]
        root_ref[own, :, my_cols] = last_root[j, root_rows(blk, rep), :]
        for copy in pending:
            copy.wait_send()
        return carry

    forward_all(0)
    lax.fori_loop(0, slots, iterate, 0)

    for j in range(slots):
        for k in range(1, reps):
            each(pieces(k, rep, 1 - side), functools.partial(wait_in, j, k))

    stores = []

    def keep(ref, hbm, f, which):
        store = pltpu.make_async_copy(ref.at[f], hbm.at[f], store_sem.at[which, len(stores)])
        store.start()
        stores.append(store)

    for j in range(slots):
        keep(inv_ref, inv_hbm, factor_of(j, rep), 0)
        for k in near_ks:
            inv_copy(j, k).wait()
            keep(inv_ref, inv_hbm, factor_of(j, source(k)), 0)
        for k in [0] + near_ks:
            for flip in range(2):
                if (k, flip) in root_ks:
                    root_copy(j, k, flip).wait()
            keep(root_ref, root_hbm, factor_of(j, source(k)), 1)
    for store in stores:
        store.wait()


def finish(root_hbm, inv_hbm, norm_ref, root_out, inv_out, held, wide, load_sem, store_sem):
    facs = root_hbm.shape[0]
    jobs = []
    for f in range(facs):
        for which, (src, dst) in enumerate(((inv_hbm, inv_out), (root_hbm, root_out))):
            load = pltpu.make_async_copy(src.at[f], held.at[which, f], load_sem.at[which, f])
            load.start()
            jobs.append((which, f, load, dst))
    stores = []
    for which, f, load, dst in jobs:
        load.wait()
        scale = jnp.sqrt(norm_ref[f : f + 1, 0:1])
        x = held[which, f].astype(jnp.float32)
        wide[which, f] = x * scale if which else x / scale
        store = pltpu.make_async_copy(wide.at[which, f], dst.at[f], store_sem.at[which, f])
        store.start()
        stores.append(store)
    for store in stores:
        store.wait()


def fused(mesh, factors, damping):
    facs, rows, order = factors.shape
    reps = mesh.shape["rep"]
    members = 2 * reps
    half = rows * reps
    slots = 2
    wide = -(-(half // 2) // LANES) * LANES
    dma = pltpu.SemaphoreType.DMA
    vmem = pl.BlockSpec(memory_space=pltpu.VMEM)
    hbm = pl.BlockSpec(memory_space=pl.ANY)
    exchanges = 2 * ITERS - 3
    bf16 = jnp.bfloat16
    root, inv, norm = pl.pallas_call(
        functools.partial(kernel, reps),
        out_shape=(
            jax.ShapeDtypeStruct(factors.shape, bf16),
            jax.ShapeDtypeStruct(factors.shape, bf16),
            jax.ShapeDtypeStruct((facs, LANES), jnp.float32),
        ),
        in_specs=[
            pl.BlockSpec(memory_space=pl.ANY),
            pl.BlockSpec(memory_space=pltpu.SMEM),
        ],
        out_specs=(hbm, hbm, vmem),
        scratch_shapes=[
            pltpu.VMEM(factors.shape, bf16),
            pltpu.VMEM(factors.shape, bf16),
            pltpu.VMEM(factors.shape, jnp.float32),
            pltpu.VMEM((members, facs, LANES), jnp.float32),
            pltpu.VMEM((facs, LANES), jnp.float32),
            pltpu.VMEM(factors.shape, bf16),
            pltpu.VMEM((slots, order, order), bf16),
            [pltpu.VMEM((slots, order, order), bf16) for _ in range(exchanges)],
            pltpu.VMEM((order, order), bf16),
            pltpu.VMEM((half, order), bf16),
            pltpu.VMEM((order, 2 * wide), bf16),
            pltpu.VMEM((slots, 2 * wide, half), bf16),
            pltpu.VMEM((slots, half // 2, order), bf16),
            dma((facs,)),
            dma((members,)), dma((members,)),
            dma((slots, reps, 2)), dma((slots, reps, 2)),
            dma((slots, reps, 2)), dma((slots, reps, 2)),
            dma((slots, exchanges, 2)), dma((slots, exchanges, 2)),
            dma((slots, reps, 2)), dma((slots, reps, 2)),
            dma((slots, reps)), dma((slots, reps)),
            dma((2, 2 * facs)),
        ],
        compiler_params=pltpu.CompilerParams(
            collective_id=0, has_side_effects=True, vmem_limit_bytes=63 * 2**20
        ),
    )(factors, damping)
    whole = jax.ShapeDtypeStruct(factors.shape, jnp.float32)
    return pl.pallas_call(
        finish,
        out_shape=(whole, whole),
        in_specs=[hbm, hbm, vmem],
        out_specs=(hbm, hbm),
        scratch_shapes=[
            pltpu.VMEM((2,) + factors.shape, bf16),
            pltpu.VMEM((2,) + factors.shape, jnp.float32),
            dma((2, facs)), dma((2, facs)),
        ],
    )(root, inv, norm)


def plain(factors, damping):
    fac_grp, row_count, order_full = factors.shape
    rep_count = lax.axis_size("rep")
    fac_rep = fac_grp // rep_count
    blk_rows = row_count * rep_count
    blk_idx = lax.axis_index("blk")
    rep_idx = lax.axis_index("rep")
    row_ids = blk_idx * blk_rows + rep_idx * row_count + lax.iota(jnp.int32, row_count)
    col_ids = lax.iota(jnp.int32, order_full)
    eye_block = (row_ids[:, None] == col_ids[None, :]).astype(jnp.float32)
    damped = factors + damping[:, None, None] * eye_block[None, :, :]
    factor_norms = jnp.sqrt(lax.psum(jnp.sum(damped * damped, axis=(1, 2)), ("rep", "blk")))
    own_rows = lax.all_to_all(damped, "rep", split_axis=0, concat_axis=1, tiled=True)
    own_norms = lax.dynamic_slice_in_dim(factor_norms, rep_idx * fac_rep, fac_rep)
    iterate = (own_rows / own_norms[:, None, None]).astype(jnp.bfloat16)
    iter_rows = blk_idx * blk_rows + lax.iota(jnp.int32, blk_rows)
    eye_rows = (iter_rows[:, None] == col_ids[None, :]).astype(jnp.float32)
    inverse = eye_rows[None, :, :].astype(jnp.bfloat16)
    for _ in range(ITERS):
        whole_iter = lax.all_gather(iterate, "blk", axis=1, tiled=True)
        whole_inv = lax.all_gather(inverse, "blk", axis=1, tiled=True)
        eye_full = jnp.eye(order_full, dtype=jnp.float32)
        moment = jnp.einsum(
            "fik,fkj->fij", whole_inv, whole_iter, preferred_element_type=jnp.float32
        )
        step = ((3.0 * eye_full[None, :, :] - moment) * 0.5).astype(jnp.bfloat16)
        step_rows = lax.dynamic_slice_in_dim(step, blk_idx * blk_rows, blk_rows, 1)
        new_iterate = jnp.einsum("fik,fkj->fij", iterate, step, preferred_element_type=jnp.float32)
        new_inverse = jnp.einsum(
            "fik,fkj->fij", step_rows, whole_inv, preferred_element_type=jnp.float32
        )
        iterate = new_iterate.astype(jnp.bfloat16)
        inverse = new_inverse.astype(jnp.bfloat16)
    root = lax.all_to_all(iterate, "rep", split_axis=1, concat_axis=0, tiled=True)
    inv = lax.all_to_all(inverse, "rep", split_axis=1, concat_axis=0, tiled=True)
    root_scale = jnp.sqrt(factor_norms)[:, None, None]
    return root.astype(jnp.float32) * root_scale, inv.astype(jnp.float32) / root_scale


def solution(mesh):
    def per_device(factors, damping):
        facs, rows, order = factors.shape
        if (
            facs == mesh.shape["rep"]
            and mesh.shape["blk"] == 2
            and rows % 16 == 0
            and facs % 2 == 0
            and (rows * facs) % LANES == 0
            and 2 * -(-(rows * facs // 2) // LANES) * LANES % CHUNK == 0
            and order % CHUNK == 0
        ):
            return fused(mesh, factors, damping)
        return plain(factors, damping)

    return jax.shard_map(
        per_device,
        mesh=mesh,
        in_specs=(P("grp", ("blk", "rep"), None), P("grp")),
        out_specs=(P("grp", ("blk", "rep"), None), P("grp", ("blk", "rep"), None)),
        check_vma=False,
    )
```

```python
import functools

import jax
import jax.numpy as jnp
from jax import lax
from jax.experimental import pallas as pl
from jax.experimental.pallas import tpu as pltpu
from jax.sharding import PartitionSpec as P

ITERS = 4
LANES = 128
CHUNK = 256
MESH = pl.DeviceIdType.MESH


def kernel(
    reps, fac_hbm, damp_ref,
    root_hbm, inv_hbm, norm_ref,
    root_ref, inv_ref, fac, part, scale, send_buf, start, held, z1, step, last_root, last_inv,
    load_sem, sum_send, sum_recv, in_send, in_recv, fwd_send, fwd_recv,
    ex_send, ex_recv, root_send, root_recv, inv_send, inv_recv, store_sem,
):
    grp = lax.axis_index("grp")
    rep = lax.axis_index("rep")
    blk = lax.axis_index("blk")
    facs, rows, order = fac.shape
    half = rows * reps
    members = 2 * reps
    rank = blk * reps + rep
    chunks = order // CHUNK
    f32, bf16 = jnp.float32, jnp.bfloat16

    side_reps = reps // 2
    side = rep // side_reps
    place = lax.rem(rep, side_reps)
    slots = facs // side_reps

    def factor_of(j, r):
        return j * side_reps + lax.rem(r, side_reps)

    def remote(src, dst, send, recv, r, b):
        return pltpu.make_async_remote_copy(
            src_ref=src, dst_ref=dst, send_sem=send, recv_sem=recv,
            device_id=(grp, r, b), device_id_type=MESH,
        )

    def member(j):
        q = lax.rem(rank + j, members)
        return lax.rem(q, reps), q // reps

    loads = [
        pltpu.make_async_copy(fac_hbm.at[f], fac.at[f], load_sem.at[f]) for f in range(facs)
    ]
    for load in loads:
        load.start()
    barrier = pltpu.get_barrier_semaphore()
    for j in range(1, members):
        r, b = member(j)
        pl.semaphore_signal(barrier, inc=1, device_id=(grp, r, b), device_id_type=MESH)

    row_ids = rank * rows + lax.broadcasted_iota(jnp.int32, (rows, order), 0)
    diag = row_ids == lax.broadcasted_iota(jnp.int32, (rows, order), 1)

    def damped(f):
        return fac[f] + jnp.where(diag, damp_ref[f], 0.0)

    for f in range(facs):
        loads[f].wait()
        x = damped(f)
        col = jnp.sum(x * x, axis=0, keepdims=True)
        acc = col[:, :LANES]
        for c in range(1, order // LANES):
            acc = acc + col[:, c * LANES : (c + 1) * LANES]
        norm_ref[f : f + 1, :] = acc
    at_lane = lax.broadcasted_iota(jnp.int32, (facs, LANES), 1)
    here = lax.broadcasted_iota(jnp.int32, (facs, LANES), 0) == at_lane
    own_sums = jnp.sum(norm_ref[...], axis=1, keepdims=True)
    part[rank] = jnp.sum(jnp.where(here, own_sums, 0.0), axis=0, keepdims=True)
    pl.semaphore_wait(barrier, members - 1)

    sums = []
    for j in range(1, members):
        r, b = member(j)
        copy = remote(part.at[rank], part.at[rank], sum_send.at[j], sum_recv.at[j], r, b)
        copy.start()
        sums.append(copy)
    for copy in sums:
        copy.wait()
    total = part[0]
    for q in range(1, members):
        total = total + part[q]
    norm = jnp.sqrt(jnp.sum(jnp.where(here, total, 0.0), axis=1, keepdims=True))
    norm_ref[...] = jnp.broadcast_to(norm, norm_ref.shape)
    scale[...] = jnp.broadcast_to(1.0 / norm, scale.shape)

    def block_rows(b, r):
        return pl.ds(pl.multiple_of((b * reps + r) * rows, rows), rows)

    wide = -(-(half // 2) // LANES) * LANES
    narrow = half - wide

    def target(k):
        if k <= side_reps:
            return (1 - side) * side_reps + lax.rem(rep + k, side_reps)
        return side * side_reps + lax.rem(rep + k, side_reps)

    def source(k):
        if k == 0:
            return rep
        back = lax.rem(rep - k + reps, side_reps)
        if k <= side_reps:
            return (1 - side) * side_reps + back
        return side * side_reps + back

    tiles = half // LANES
    widths = sorted({tiles - (r * rows) // LANES for r in range(side_reps, reps)})

    def width_of(r, owner_side):
        mirrored = r + owner_side * (reps - 1 - 2 * r)
        return tiles - (mirrored * rows) // LANES

    def pieces(k, src, owner_side):
        if k == 0 or k > side_reps:
            return [(None, [pl.ds(0, order)])]
        options = []
        for w in widths:
            first = (1 - owner_side) * (half - w * LANES)
            options.append((
                width_of(src, owner_side) == w,
                [pl.ds(pl.multiple_of(h * half + first, LANES), w * LANES) for h in range(2)],
            ))
        return options

    def each(options, act):
        for condition, columns in options:
            if condition is None:
                act(columns)
            else:
                pl.when(condition)(functools.partial(act, columns))

    own_rows = block_rows(blk, rep)
    far_ks = list(range(1, side_reps + 1))
    near_ks = list(range(side_reps + 1, reps))

    def start_of(j):
        return start.at[j]

    def in_copy(j, k, i, c):
        p = target(k)
        return remote(
            send_buf.at[factor_of(j, p), :, c], start_of(j).at[own_rows, c],
            in_send.at[j, k, i], in_recv.at[j, k, i], p, blk,
        )

    def send_in(j, k, columns):
        for i, c in enumerate(columns):
            in_copy(j, k, i, c).start()

    def wait_in(j, k, columns):
        for i, c in enumerate(columns):
            in_copy(j, k, i, c).wait_send()

    def round_rows(j, k):
        p = factor_of(j, target(k))
        rounded = (damped(p) * scale[pl.ds(p, 1), 0:1]).astype(bf16)
        send_buf[p] = rounded
        if k == side_reps:
            start_of(j)[own_rows, :] = rounded

    def send_all(j, ks):
        for k in ks:
            each(pieces(k, rep, 1 - side), functools.partial(send_in, j, k))

    for k in far_ks:
        round_rows(0, k)
        send_all(0, [k])
    send_all(0, near_ks)
    for j in range(1, slots):
        for k in far_ks:
            round_rows(j, k)

    def forward_copy(j, k, i, c):
        at = block_rows(blk, source(k))
        y0 = start_of(j)
        return remote(
            y0.at[at, c], y0.at[at, c], fwd_send.at[j, k, i], fwd_recv.at[j, k, i],
            rep, 1 - blk,
        )

    def forward(j, k, columns):
        for i, c in enumerate(columns):
            if k:
                in_copy(j, k, i, c).wait_recv()
            forward_copy(j, k, i, c).start()

    def wait_forward(j, k, columns):
        for i, c in enumerate(columns):
            forward_copy(j, k, i, c).wait()

    def forward_all(j):
        for k in [0] + near_ks + far_ks:
            each(pieces(k, source(k), side), functools.partial(forward, j, k))

    far = half // 2
    miss = half - min(widths) * LANES

    def fill(t, old, row0, col0, mirrored):
        shape = (far, miss)
        r = (row0 + lax.broadcasted_iota(jnp.int32, shape, 0)) // rows
        c = (col0 + lax.broadcasted_iota(jnp.int32, shape, 1)) // LANES
        if mirrored:
            gone = c >= tiles - ((reps - 1 - r) * rows) // LANES
        else:
            gone = c < (r * rows) // LANES
        return jnp.where(gone, t, old.astype(f32)).astype(bf16)

    mine = pl.ds(pl.multiple_of(blk * half, half), half)
    my_cols = pl.ds(pl.multiple_of(blk * half, LANES), half)
    near_rows = pl.ds(pl.multiple_of(side * far, far), far)
    eye_rows = blk * half + lax.broadcasted_iota(jnp.int32, (half, CHUNK), 0)
    eye_cols = lax.broadcasted_iota(jnp.int32, (half, CHUNK), 1)

    whole = [(0, chunks)]
    halves = [(0, (chunks + 1) // 2), ((chunks + 1) // 2, chunks)]

    def cols(n):
        return slice(n * CHUNK, (n + 1) * CHUNK)

    def inv_copy(j, k):
        p = target(k)
        at = pl.ds(pl.multiple_of(lax.rem(p, side_reps) * rows, rows), rows)
        return remote(
            last_inv.at[j, at], inv_ref.at[factor_of(j, rep)],
            inv_send.at[j, k], inv_recv.at[j, k], p, blk,
        )

    def root_rows(b, r):
        first = b * wide + side * (far - narrow) + lax.rem(r, side_reps) * rows
        return pl.ds(pl.multiple_of(first, 16), rows)

    def root_copy(j, k, flip):
        r = target(k) if k else rep
        b = blk + flip - 2 * blk * flip
        return remote(
            last_root.at[j, root_rows(b, r)], root_ref.at[factor_of(j, rep), :, my_cols],
            root_send.at[j, k, flip], root_recv.at[j, k, flip], r, b,
        )

    root_ks = [(k, flip) for k in near_ks for flip in range(2)] + [(0, 1)]

    def iterate(j, carry):
        for k in range(reps):
            each(pieces(k, source(k), side), functools.partial(wait_forward, j, k))
        y0 = start_of(j)

        @pl.when(j + 1 < slots)
        def _():
            send_all(j + 1, far_ks + near_ks)

        @pl.when(side == 0)
        def _():
            for hi in range(2):
                for hj in range(2):
                    t = y0[hj * half : hj * half + miss, hi * half + narrow : (hi + 1) * half]
                    at = (
                        slice(hi * half + far, (hi + 1) * half),
                        slice(hj * half, hj * half + miss),
                    )
                    t = t.astype(f32).T[far - narrow :, :]
                    y0[at] = fill(t, y0[at], far, 0, False)

        @pl.when(side == 1)
        def _():
            for hi in range(2):
                for hj in range(2):
                    t = y0[(hj + 1) * half - miss : (hj + 1) * half, hi * half : hi * half + wide]
                    at = (
                        slice(hi * half, hi * half + far),
                        slice((hj + 1) * half - miss, (hj + 1) * half),
                    )
                    t = t.astype(f32).T[:far, :]
                    y0[at] = fill(t, y0[at], 0, half - miss, True)

        for n in range(chunks):
            eye = jnp.where(eye_rows == eye_cols + n * CHUNK, 3.0, 0.0)
            step[:, cols(n)] = ((eye - y0[mine, cols(n)].astype(f32)) * 0.5).astype(bf16)
        pending = []

        def share(dst, ex, part, first, last):
            view = dst.at[mine, pl.ds(first * CHUNK, (last - first) * CHUNK)]
            copy = remote(
                view, view, ex_send.at[j, ex, part], ex_recv.at[j, ex, part], rep, 1 - blk
            )
            copy.start()
            pending.append(copy)
            return copy

        def settle(arrivals):
            for copy in arrivals:
                copy.wait_recv()

        def product(lhs, rhs, n):
            return jnp.dot(lhs, rhs[:, cols(n)], preferred_element_type=f32)

        def advance(lhs, rhs, arrivals, dst, ex, parts):
            settle(arrivals)
            shared = []
            for part, (first, last) in enumerate(parts):
                for n in range(first, last):
                    dst[mine, cols(n)] = product(lhs[...], rhs, n).astype(bf16)
                shared.append(share(dst, ex, part, first, last))
            return shared

        def make_step(y, z, arrivals):
            settle(arrivals)
            for n in range(chunks):
                moment = product(y[mine, :], z, n)
                eye = jnp.where(eye_rows == eye_cols + n * CHUNK, 3.0, 0.0)
                step[:, cols(n)] = ((eye - moment) * 0.5).astype(bf16)

        def make_step_rows(y, z, first, count):
            first = pl.multiple_of(first, 16)
            top = pl.multiple_of(blk * half + first, 16)
            ids = top + lax.broadcasted_iota(jnp.int32, (count, CHUNK), 0)
            for n in range(chunks):
                moment = product(y[pl.ds(top, count), :], z, n)
                at = n * CHUNK + lax.broadcasted_iota(jnp.int32, (count, CHUNK), 1)
                eye = jnp.where(ids == at, 3.0, 0.0)
                step[pl.ds(first, count), cols(n)] = ((eye - moment) * 0.5).astype(bf16)

        y, z, z_in = held[0].at[j], z1, []
        y_in = advance(step, y0, [], y, 0, whole)
        for q in range(members):
            at = slice(q * rows, (q + 1) * rows)
            ids = q * rows + lax.broadcasted_iota(jnp.int32, (rows, order), 0)
            eye = ids == lax.broadcasted_iota(jnp.int32, (rows, order), 1)
            z1[at, :] = ((jnp.where(eye, 3.0, 0.0) - y0[at, :].astype(f32)) * 0.5).astype(bf16)

        ex = 1
        for _ in range(ITERS - 2):
            make_step(y, z, z_in)
            z_next, y_next = held[ex].at[j], held[ex + 1].at[j]
            z_in_next = advance(step, z, [], z_next, ex, halves)
            y_in = advance(step, y, y_in, y_next, ex + 1, whole)
            y, z, z_in = y_next, z_next, z_in_next
            ex = ex + 2
        settle(z_in)
        make_step_rows(y, z, side * far, far)
        for n in range(chunks):
            last_inv[j, :, cols(n)] = product(step[near_rows, :], z, n).astype(bf16)
        for k in near_ks:
            inv_copy(j, k).start()

        @pl.when(j + 1 < slots)
        def _():
            forward_all(j + 1)

        make_step_rows(y, z, (1 - side) * far, far)
        settle(y_in)
        for h in range(2):
            at = pl.ds(pl.multiple_of(h * half + side * narrow, LANES), wide)
            z1[:, h * wide : (h + 1) * wide] = y[:, at]
        for n in range(2 * wide // CHUNK):
            out = product(step[...], z1, n)
            last_root[j, cols(n), :] = out.T.astype(bf16)
        for k, flip in root_ks:
            root_copy(j, k, flip).start()
        own = factor_of(j, rep)
        local = pl.ds(pl.multiple_of(place * rows, rows), rows)
        inv_ref[own] = last_inv[j, local, :]
        root_ref[own, :, my_cols] = last_root[j, root_rows(blk, rep), :]
        for copy in pending:
            copy.wait_send()
        return carry

    forward_all(0)
    lax.fori_loop(0, slots, iterate, 0)

    for j in range(slots):
        for k in range(1, reps):
            each(pieces(k, rep, 1 - side), functools.partial(wait_in, j, k))

    stores = []

    def keep(ref, hbm, f, which):
        store = pltpu.make_async_copy(ref.at[f], hbm.at[f], store_sem.at[which, len(stores)])
        store.start()
        stores.append(store)

    for j in range(slots):
        keep(inv_ref, inv_hbm, factor_of(j, rep), 0)
        for k in near_ks:
            inv_copy(j, k).wait()
            keep(inv_ref, inv_hbm, factor_of(j, source(k)), 0)
        for k in [0] + near_ks:
            for flip in range(2):
                if (k, flip) in root_ks:
                    root_copy(j, k, flip).wait()
            keep(root_ref, root_hbm, factor_of(j, source(k)), 1)
    for store in stores:
        store.wait()


def finish(root_hbm, inv_hbm, norm_ref, root_out, inv_out, held, wide, load_sem, store_sem):
    facs = root_hbm.shape[0]
    jobs = []
    for f in range(facs):
        for which, (src, dst) in enumerate(((inv_hbm, inv_out), (root_hbm, root_out))):
            load = pltpu.make_async_copy(src.at[f], held.at[which, f], load_sem.at[which, f])
            load.start()
            jobs.append((which, f, load, dst))
    stores = []
    for which, f, load, dst in jobs:
        load.wait()
        scale = jnp.sqrt(norm_ref[f : f + 1, 0:1])
        x = held[which, f].astype(jnp.float32)
        wide[which, f] = x * scale if which else x / scale
        store = pltpu.make_async_copy(wide.at[which, f], dst.at[f], store_sem.at[which, f])
        store.start()
        stores.append(store)
    for store in stores:
        store.wait()


def fused(mesh, factors, damping):
    facs, rows, order = factors.shape
    reps = mesh.shape["rep"]
    members = 2 * reps
    half = rows * reps
    slots = 2
    wide = -(-(half // 2) // LANES) * LANES
    dma = pltpu.SemaphoreType.DMA
    vmem = pl.BlockSpec(memory_space=pltpu.VMEM)
    hbm = pl.BlockSpec(memory_space=pl.ANY)
    exchanges = 2 * ITERS - 3
    bf16 = jnp.bfloat16
    root, inv, norm = pl.pallas_call(
        functools.partial(kernel, reps),
        out_shape=(
            jax.ShapeDtypeStruct(factors.shape, bf16),
            jax.ShapeDtypeStruct(factors.shape, bf16),
            jax.ShapeDtypeStruct((facs, LANES), jnp.float32),
        ),
        in_specs=[
            pl.BlockSpec(memory_space=pl.ANY),
            pl.BlockSpec(memory_space=pltpu.SMEM),
        ],
        out_specs=(hbm, hbm, vmem),
        scratch_shapes=[
            pltpu.VMEM(factors.shape, bf16),
            pltpu.VMEM(factors.shape, bf16),
            pltpu.VMEM(factors.shape, jnp.float32),
            pltpu.VMEM((members, 1, LANES), jnp.float32),
            pltpu.VMEM((facs, LANES), jnp.float32),
            pltpu.VMEM(factors.shape, bf16),
            pltpu.VMEM((slots, order, order), bf16),
            [pltpu.VMEM((slots, order, order), bf16) for _ in range(exchanges)],
            pltpu.VMEM((order, order), bf16),
            pltpu.VMEM((half, order), bf16),
            pltpu.VMEM((slots, 2 * wide, half), bf16),
            pltpu.VMEM((slots, half // 2, order), bf16),
            dma((facs,)),
            dma((members,)), dma((members,)),
            dma((slots, reps, 2)), dma((slots, reps, 2)),
            dma((slots, reps, 2)), dma((slots, reps, 2)),
            dma((slots, exchanges, 2)), dma((slots, exchanges, 2)),
            dma((slots, reps, 2)), dma((slots, reps, 2)),
            dma((slots, reps)), dma((slots, reps)),
            dma((2, 2 * facs)),
        ],
        compiler_params=pltpu.CompilerParams(
            collective_id=0, has_side_effects=True, vmem_limit_bytes=63 * 2**20
        ),
    )(factors, damping)
    whole = jax.ShapeDtypeStruct(factors.shape, jnp.float32)
    return pl.pallas_call(
        finish,
        out_shape=(whole, whole),
        in_specs=[hbm, hbm, vmem],
        out_specs=(hbm, hbm),
        scratch_shapes=[
            pltpu.VMEM((2,) + factors.shape, bf16),
            pltpu.VMEM((2,) + factors.shape, jnp.float32),
            dma((2, facs)), dma((2, facs)),
        ],
    )(root, inv, norm)


def plain(factors, damping):
    fac_grp, row_count, order_full = factors.shape
    rep_count = lax.axis_size("rep")
    fac_rep = fac_grp // rep_count
    blk_rows = row_count * rep_count
    blk_idx = lax.axis_index("blk")
    rep_idx = lax.axis_index("rep")
    row_ids = blk_idx * blk_rows + rep_idx * row_count + lax.iota(jnp.int32, row_count)
    col_ids = lax.iota(jnp.int32, order_full)
    eye_block = (row_ids[:, None] == col_ids[None, :]).astype(jnp.float32)
    damped = factors + damping[:, None, None] * eye_block[None, :, :]
    factor_norms = jnp.sqrt(lax.psum(jnp.sum(damped * damped, axis=(1, 2)), ("rep", "blk")))
    own_rows = lax.all_to_all(damped, "rep", split_axis=0, concat_axis=1, tiled=True)
    own_norms = lax.dynamic_slice_in_dim(factor_norms, rep_idx * fac_rep, fac_rep)
    iterate = (own_rows / own_norms[:, None, None]).astype(jnp.bfloat16)
    iter_rows = blk_idx * blk_rows + lax.iota(jnp.int32, blk_rows)
    eye_rows = (iter_rows[:, None] == col_ids[None, :]).astype(jnp.float32)
    inverse = eye_rows[None, :, :].astype(jnp.bfloat16)
    for _ in range(ITERS):
        whole_iter = lax.all_gather(iterate, "blk", axis=1, tiled=True)
        whole_inv = lax.all_gather(inverse, "blk", axis=1, tiled=True)
        eye_full = jnp.eye(order_full, dtype=jnp.float32)
        moment = jnp.einsum(
            "fik,fkj->fij", whole_inv, whole_iter, preferred_element_type=jnp.float32
        )
        step = ((3.0 * eye_full[None, :, :] - moment) * 0.5).astype(jnp.bfloat16)
        step_rows = lax.dynamic_slice_in_dim(step, blk_idx * blk_rows, blk_rows, 1)
        new_iterate = jnp.einsum("fik,fkj->fij", iterate, step, preferred_element_type=jnp.float32)
        new_inverse = jnp.einsum(
            "fik,fkj->fij", step_rows, whole_inv, preferred_element_type=jnp.float32
        )
        iterate = new_iterate.astype(jnp.bfloat16)
        inverse = new_inverse.astype(jnp.bfloat16)
    root = lax.all_to_all(iterate, "rep", split_axis=1, concat_axis=0, tiled=True)
    inv = lax.all_to_all(inverse, "rep", split_axis=1, concat_axis=0, tiled=True)
    root_scale = jnp.sqrt(factor_norms)[:, None, None]
    return root.astype(jnp.float32) * root_scale, inv.astype(jnp.float32) / root_scale


def solution(mesh):
    def per_device(factors, damping):
        facs, rows, order = factors.shape
        if (
            facs == mesh.shape["rep"]
            and mesh.shape["blk"] == 2
            and rows % 16 == 0
            and facs % 2 == 0
            and (rows * facs) % LANES == 0
            and 2 * -(-(rows * facs // 2) // LANES) * LANES % CHUNK == 0
            and order % CHUNK == 0
        ):
            return fused(mesh, factors, damping)
        return plain(factors, damping)

    return jax.shard_map(
        per_device,
        mesh=mesh,
        in_specs=(P("grp", ("blk", "rep"), None), P("grp")),
        out_specs=(P("grp", ("blk", "rep"), None), P("grp", ("blk", "rep"), None)),
        check_vma=False,
    )
```
